16 devices in a mesh: dp: 2 (over y, z), tp: 8 (over x, core).
Axes of the slice: x: 4, y: 2, z: 1, core: 2. Of those that a mesh axis runs over, the one named last changes fastest.
The devices are a block of a 4x4x8 slice.
Arguments:
- x: bfloat16 [8192, 2048], P(('dp', 'tp')), parts along dimension 0
- dy: bfloat16 [8192, 2048], P(('dp', 'tp')), parts along dimension 0
- gate: bfloat16 [8192, 5120], P('dp', 'tp'), parts along dimension 0
- up: bfloat16 [8192, 5120], P('dp', 'tp'), parts along dimension 0
- w_gate: bfloat16 [2048, 5120], P(None, 'tp')
- w_up: bfloat16 [2048, 5120], P(None, 'tp')
- w_down: bfloat16 [5120, 2048], P('tp')
Outputs:
- output 1: bfloat16 [8192, 2048], P(('dp', 'tp')), parts along dimension 0
- output 2: bfloat16 [4096, 5120], P('dp', 'tp'), parts along dimension 0
- output 3: bfloat16 [4096, 5120], P('dp', 'tp'), parts along dimension 0
- output 4: bfloat16 [10240, 2048], P(('dp', 'tp')), parts along dimension 0
There are 2 independent parts. The reference program is written for one: setup_inputs(seed, part) draws one part's arguments, and reference() takes and returns one part's arrays. A program takes and returns all parts, laid end to end along the dimension named above; an argument that names none is the same for every part.
All inputs are finite; a program needn't handle non-finite values.
Results may differ from the reference program's by a relative error of at most 0.012.
Values are sent between devices in bfloat16 or wider.
A program may use at most 768 MiB of HBM per device.

```python
import jax
import jax.numpy as jnp

ROWS = 4096
D = 2048
FF = 5120


def act(gate, up):
    return jax.nn.gelu(gate) * up


def setup_inputs(seed: int = 0, part: int = 0) -> dict:
    kx, ky, ka, kb, kg, ku, kd = jax.random.split(jax.random.key(seed), 7)
    kx, ky, ka, kb = (jax.random.fold_in(k, part) for k in (kx, ky, ka, kb))
    drawn = {
        "x": jax.random.normal(kx, (ROWS, D), jnp.float32),
        "dy": jax.random.normal(ky, (ROWS, D), jnp.float32),
        "gate": jax.random.normal(ka, (ROWS, FF), jnp.float32),
        "up": jax.random.normal(kb, (ROWS, FF), jnp.float32),
        "w_gate": jax.random.normal(kg, (D, FF), jnp.float32) * D**-0.5,
        "w_up": jax.random.normal(ku, (D, FF), jnp.float32) * D**-0.5,
        "w_down": jax.random.normal(kd, (FF, D), jnp.float32) * FF**-0.5,
    }
    return {k: v.astype(jnp.bfloat16) for k, v in drawn.items()}


def reference(x, dy, gate, up, w_gate, w_up, w_down):
    hidden, back = jax.vjp(act, gate.astype(jnp.float32), up.astype(jnp.float32))
    d_hidden = jnp.dot(dy, w_down.T, preferred_element_type=jnp.float32)
    d_gate, d_up = (g.astype(jnp.bfloat16) for g in back(d_hidden))
    dx = jnp.dot(d_gate, w_gate.T, preferred_element_type=jnp.float32) + jnp.dot(d_up, w_up.T, preferred_element_type=jnp.float32)
    dw_gate = jnp.dot(x.T, d_gate, preferred_element_type=jnp.float32)
    dw_up = jnp.dot(x.T, d_up, preferred_element_type=jnp.float32)
    dw_down = jnp.dot(hidden.astype(jnp.bfloat16).T, dy, preferred_element_type=jnp.float32)
    return tuple(g.astype(jnp.bfloat16) for g in (dx, dw_gate, dw_up, dw_down))
```

```python
import functools

import jax
import jax.numpy as jnp
from jax import lax
from jax.experimental import pallas as pl
from jax.experimental.pallas import tpu as pltpu
from jax.sharding import PartitionSpec as P

MESH = pl.DeviceIdType.MESH
BF16, F32 = jnp.bfloat16, jnp.float32
NT = (((1,), (1,)), ((), ()))
TN = (((0,), (0,)), ((), ()))


def act(gate, up):
    return jax.nn.gelu(gate) * up


def kernel(
    n, x_ref, dy_ref, gate_ref, up_ref, wg_ref, wu_ref, wd_ref,
    dx_ref, dwg_ref, dwu_ref, dwd_ref, dyg, xg, pbuf,
    wd_v, wgu_v, dgu_v, hid_v, tile_v, gu_v, dh_v, psend, rsend, rrecv, acc_v, strip_v, so_v, sd_v,
    ag_s, ag_r, p_s, p_r, q_s, q_r, w_sem, g_sem, t_sem, own_sem, st_sem, so_sem, sd_sem, dx_sem,
):
    me = lax.axis_index("tp")
    core = lax.rem(me, 2)
    other = 1 - 2 * core
    right, left, far = lax.rem(me + 2, n), lax.rem(me + n - 2, n), lax.rem(me + 4, n)
    partner = me + other
    R, D = dy_ref.shape
    H = R // 2
    F = gate_ref.shape[1]
    T = n * R

    def rows(block, half=None):
        if half is None:
            return pl.ds(pl.multiple_of(block * R, R), R)
        return pl.ds(pl.multiple_of(block * R + half * H, H), H)

    def local(src, dst, sem):
        return pltpu.make_async_copy(src, dst, sem)

    def remote(src, dst, s, r, to):
        return pltpu.make_async_remote_copy(src_ref=src, dst_ref=dst, send_sem=s, recv_sem=r, device_id={"tp": to}, device_id_type=MESH)

    pieces = ((left, 0), (left, 1), (right, 1), (right, 0), (far, 0), (far, 1))
    own_sends = ((right, 0), (right, 1), (left, 1), (left, 0))
    own = (dy_ref, x_ref)
    full = (dyg, xg)

    def ring_own(a, k):
        to, half = own_sends[k]
        return remote(own[a].at[pl.ds(half * H, H)], full[a].at[rows(me, half)], ag_s.at[a, k], ag_r.at[a, k], to)

    def ring_fwd(a, k):
        block, half, to = ((left, 0, right), (right, 1, left))[k - 4]
        ref = full[a].at[rows(block, half)]
        return remote(ref, ref, ag_s.at[a, k], ag_r.at[a, k], to)

    def ring_arrived(a, k):
        block, half = pieces[k]
        ref = full[a].at[rows(block, half)]
        remote(ref, ref, ag_s.at[a, k], ag_r.at[a, k], partner).wait_recv()

    def pair_own(a):
        return remote(own[a], full[a].at[rows(me)], ag_s.at[a, 6], ag_r.at[a, 6], partner)

    def pair_fwd(a, k):
        block, half = pieces[k]
        ref = full[a].at[rows(block, half)]
        return remote(ref, ref, ag_s.at[a, 7 + k], ag_r.at[a, 7 + k], partner)

    def pair_arrived(a, k):
        if k < 0:
            ref = full[a].at[rows(partner)]
            remote(ref, ref, ag_s.at[a, 6], ag_r.at[a, 6], partner).wait_recv()
        else:
            block, half = pieces[k]
            ref = full[a].at[rows(block + other, half)]
            remote(ref, ref, ag_s.at[a, 7 + k], ag_r.at[a, 7 + k], partner).wait_recv()

    w_copies = (
        local(wd_ref, wd_v, w_sem.at[0]),
        local(wg_ref, wgu_v.at[:, pl.ds(0, F)], w_sem.at[1]),
        local(wu_ref, wgu_v.at[:, pl.ds(F, F)], w_sem.at[2]),
    )

    barrier = pltpu.get_barrier_semaphore()
    for to in (left, right, partner):
        pl.semaphore_signal(barrier, inc=1, device_id={"tp": to}, device_id_type=MESH)
    pl.semaphore_wait(barrier, 3)

    for k in (0, 2, 1, 3):
        ring_own(0, k).start()
    pair_own(0).start()
    pair_own(1).start()

    def block_of(s):
        j = s // 2
        hop = j + j // 2 - 2 * (j // 3)
        return lax.rem(me + 2 * hop, n) + lax.rem(s, 2) * other

    def gate_load(s, slot):
        r = rows(block_of(s))
        return (
            local(gate_ref.at[r], gu_v.at[slot, 0], g_sem.at[slot, 0]),
            local(up_ref.at[r], gu_v.at[slot, 1], g_sem.at[slot, 1]),
        )

    def tile_load(s, slot):
        return local(dyg.at[rows(block_of(s))], tile_v.at[slot], t_sem.at[slot])

    w_copies[0].start()
    local(dy_ref, tile_v.at[0], t_sem.at[0]).start()
    for c in gate_load(0, 0):
        c.start()
    stage = [local(dy_ref, psend.at[0], own_sem.at[0]), local(x_ref, psend.at[1], own_sem.at[1])]
    for c in stage:
        c.start()
    w_copies[1].start()
    w_copies[2].start()
    for c in stage:
        c.wait()
    stage = [local(psend.at[0], dyg.at[rows(me)], own_sem.at[0]), local(psend.at[1], xg.at[rows(me)], own_sem.at[1])]
    for c in stage:
        c.start()
    w_copies[0].wait()

    def step(s, _):
        slot, nxt = lax.rem(s, 2), lax.rem(s + 1, 2)
        r = rows(block_of(s))
        tile_load(s, slot).wait()
        for c in gate_load(s, slot):
            c.wait()
        dh_v[...] = lax.dot_general(tile_v[slot], wd_v[...], NT, preferred_element_type=F32)

        @pl.when(s == 0)
        def _():
            pair_arrived(0, -1)

        @pl.when(s == 1)
        def _():
            for k in (0, 2):
                ring_arrived(0, k)
            for k in (4, 5):
                ring_fwd(0, k).start()
            for k in (0, 2, 1, 3):
                ring_own(1, k).start()
            for k in (0, 2):
                pair_fwd(0, k).start()
            for k in (1, 3):
                ring_arrived(0, k)
                pair_fwd(0, k).start()

        @pl.when(s == 2)
        def _():
            for k in (2, 3):
                pair_arrived(0, k)

        @pl.when(s == 4)
        def _():
            for k in (0, 1):
                pair_arrived(0, k)

        @pl.when(s == 5)
        def _():
            for k in (4, 5):
                ring_arrived(0, k)
                pair_fwd(0, k).start()

        @pl.when(s == 6)
        def _():
            for k in (4, 5):
                pair_arrived(0, k)

        @pl.when(s < n - 1)
        def _():
            tile_load(s + 1, nxt).start()
            for c in gate_load(s + 1, nxt):
                c.start()

        def chunk(i, _):
            m = 16
            q = pl.ds(pl.multiple_of(i * m, m), m)
            o = pl.ds(pl.multiple_of(block_of(s) * R + i * m, m), m)
            hidden, back = jax.vjp(act, gu_v[slot, 0, q].astype(F32), gu_v[slot, 1, q].astype(F32))
            dg, du = back(dh_v[q])
            dgu_v[o, pl.ds(0, F)] = dg.astype(BF16)
            dgu_v[o, pl.ds(F, F)] = du.astype(BF16)
            hid_v[o] = hidden.astype(BF16)
            return 0

        lax.fori_loop(0, R // 16, chunk, 0)
        return 0

    lax.fori_loop(0, n, step, 0)
    for c in stage:
        c.wait()
    for c in w_copies[1:]:
        c.wait()

    NB = 512

    def dx_terms(row0, m, emit):
        def ntile(t, _):
            cols = pl.ds(pl.multiple_of(t * NB, NB), NB)
            emit(cols, lax.dot_general(dgu_v[pl.ds(row0, m)], wgu_v[cols], NT, preferred_element_type=F32))
            return 0

        lax.fori_loop(0, D // NB, ntile, 0)

    targets = (far, right, left, me)

    def p_copy(i):
        return remote(psend.at[i % 2], pbuf.at[i], p_s.at[i], p_r.at[i], partner)

    for i, block in enumerate(targets):
        if i >= 2:
            p_copy(i - 2).wait_send()

        def emit(cols, v, i=i):
            psend[i % 2, :, cols] = v.astype(BF16)

        dx_terms(pl.multiple_of((block + other) * R, R), R, emit)
        p_copy(i).start()

    for k in (0, 2):
        ring_arrived(1, k)
    for k in (4, 5):
        ring_fwd(1, k).start()
    for k in (0, 2):
        pair_fwd(1, k).start()

    def p_load(i, half=None):
        if half is None:
            return local(pbuf.at[i], tile_v.at[i % 2], t_sem.at[i % 2])
        h = pl.ds(half * H, H)
        return local(pbuf.at[i, h], tile_v.at[i % 2, h], t_sem.at[i % 2])

    def p_fetch(i):
        p_copy(i).wait_recv()
        p_load(i).start()

    def q_sub(q, sub, subs):
        to = (right, left)[q % 2]
        h = pl.ds(sub * (H // subs), H // subs)
        k = q + 2 * sub
        return remote(rsend.at[q, h], rrecv.at[q, h], q_s.at[k], q_r.at[k], to)

    def q_parts(q):
        return [q_sub(q, sub, 2 if q >= 4 else 1) for sub in range(2 if q >= 4 else 1)]

    def ring_sum(q, i, half, add=None):
        h = pl.ds(half * H, H)

        def emit(cols, v):
            v = v + tile_v[i % 2, h, cols].astype(F32)
            if add is not None:
                v = v + rrecv[add, :, cols].astype(F32)
            rsend[q, :, cols] = v.astype(BF16)

        dx_terms(pl.multiple_of(targets[i] * R + half * H, H), H, emit)
        for c in q_parts(q):
            c.start()

    p_fetch(0)
    p_fetch(1)
    p_load(0).wait()
    ring_sum(0, 0, 0)
    ring_sum(1, 0, 1)
    p_fetch(2)
    p_load(1).wait()
    ring_sum(2, 1, 1)
    p_fetch(3)
    p_load(2).wait()
    ring_sum(3, 2, 0)
    p_load(3).wait()

    def emit_own(cols, v):
        acc_v[:, cols] = v + tile_v[1, :, cols].astype(F32)

    dx_terms(pl.multiple_of(me * R, R), R, emit_own)

    for k in (1, 3):
        ring_arrived(1, k)
        pair_fwd(1, k).start()

    W = strip_v.shape[2]

    def strip_load(a, t, slot):
        return local(full[a].at[:, pl.ds(pl.multiple_of(t * W, W), W)], strip_v.at[slot], st_sem.at[slot])

    def strips(a, lo, hi, out, work):
        strip_load(a, lo, lo % 2).start()

        def one(t, _):
            slot = lax.rem(t, 2)
            strip_load(a, t, slot).wait()

            @pl.when(t + 1 < hi)
            def _():
                strip_load(a, t + 1, 1 - slot).start()

            @pl.when(t >= lo + 2)
            def _():
                for c in out(t - 2, slot):
                    c.wait()

            work(slot)
            for c in out(t, slot):
                c.start()
            return 0

        lax.fori_loop(lo, hi, one, 0)
        for t in (hi - 2, hi - 1):
            for c in out(t, t % 2):
                c.wait()

    def down_out(t, slot):
        return (local(sd_v.at[slot], dwd_ref.at[:, pl.ds(pl.multiple_of(t * W, W), W)], sd_sem.at[slot]),)

    def down_work(slot):
        v = lax.dot_general(strip_v[slot], hid_v[...], TN, preferred_element_type=F32)
        sd_v[slot] = v.T.astype(BF16)

    def in_out(t, slot):
        r = pl.ds(pl.multiple_of(t * W, W), W)
        return (
            local(so_v.at[slot, :, pl.ds(0, F)], dwg_ref.at[r], so_sem.at[slot, 0]),
            local(so_v.at[slot, :, pl.ds(F, F)], dwu_ref.at[r], so_sem.at[slot, 1]),
        )

    def in_work(slot):
        v = lax.dot_general(strip_v[slot], dgu_v[...], TN, preferred_element_type=F32)
        so_v[slot] = v.astype(BF16)

    S = D // W
    strips(0, 0, S, down_out, down_work)

    for k in (4, 5):
        ring_arrived(1, k)
        pair_fwd(1, k).start()
    for k in (-1, 0, 1, 2, 3, 4, 5):
        pair_arrived(1, k)

    strips(1, 0, S // 2, in_out, in_work)

    for i, half in ((1, 0), (2, 1)):
        p_load(i, half).start()
    for c in q_parts(0) + q_parts(1):
        c.wait_recv()
    for i, half in ((1, 0), (2, 1)):
        p_load(i, half).wait()
    ring_sum(4, 1, 0, add=0)
    ring_sum(5, 2, 1, add=1)

    strips(1, S // 2, S, in_out, in_work)

    def add_rows(lo, m, srcs):
        def chunk(i, _):
            r = pl.ds(pl.multiple_of(lo + i * 16, 16), 16)
            v = acc_v[r]
            for q in srcs:
                v = v + rrecv[q, pl.ds(pl.multiple_of(lo % H + i * 16, 16), 16)].astype(F32)
            return r, v

        return chunk

    for c in q_parts(2) + q_parts(3):
        c.wait_recv()

    outs = []
    for sub in range(2):
        for q, first, base in ((4, 3, 0), (5, 2, H)):
            q_parts(q)[sub].wait_recv()
            lo = base + sub * (H // 2)
            chunk = add_rows(lo, H // 2, (first, q))

            def put(i, _, chunk=chunk):
                r, v = chunk(i, _)
                tile_v[0, r] = v.astype(BF16)
                return 0

            lax.fori_loop(0, H // 2 // 16, put, 0)
            r = pl.ds(lo, H // 2)
            out = local(tile_v.at[0, r], dx_ref.at[r], dx_sem.at[len(outs)])
            out.start()
            outs.append(out)

    for a in range(2):
        for k in range(4):
            ring_own(a, k).wait_send()
        for k in (4, 5):
            ring_fwd(a, k).wait_send()
        pair_own(a).wait_send()
        for k in range(6):
            pair_fwd(a, k).wait_send()
    for i in (2, 3):
        p_copy(i).wait_send()
    for q in range(6):
        for c in q_parts(q):
            c.wait_send()
    for c in outs:
        c.wait()


def solution(mesh):
    n = mesh.shape["tp"]

    def body(x, dy, gate, up, w_gate, w_up, w_down):
        R, D = x.shape
        T, F = gate.shape
        H = R // 2
        W = 256
        out = lambda *s: jax.ShapeDtypeStruct(s, BF16)
        any_spec = pl.BlockSpec(memory_space=pl.ANY)
        dma = pltpu.SemaphoreType.DMA
        res = pl.pallas_call(
            functools.partial(kernel, n),
            out_shape=[out(R, D), out(D, F), out(D, F), out(F, D), out(T, D), out(T, D), out(4, R, D)],
            in_specs=[any_spec] * 7,
            out_specs=[any_spec] * 7,
            scratch_shapes=[
                pltpu.VMEM((F, D), BF16),
                pltpu.VMEM((D, 2 * F), BF16),
                pltpu.VMEM((T, 2 * F), BF16),
                pltpu.VMEM((T, F), BF16),
                pltpu.VMEM((2, R, D), BF16),
                pltpu.VMEM((2, 2, R, F), BF16),
                pltpu.VMEM((R, F), F32),
                pltpu.VMEM((2, R, D), BF16),
                pltpu.VMEM((6, H, D), BF16),
                pltpu.VMEM((6, H, D), BF16),
                pltpu.VMEM((R, D), F32),
                pltpu.VMEM((2, T, W), BF16),
                pltpu.VMEM((2, W, 2 * F), BF16),
                pltpu.VMEM((2, F, W), BF16),
                dma((2, 13)), dma((2, 13)),
                dma((4,)), dma((4,)),
                dma((8,)), dma((8,)),
                dma((3,)), dma((2, 2)), dma((2,)), dma((2,)),
                dma((2,)), dma((2, 2)), dma((2,)), dma((4,)),
            ],
            compiler_params=pltpu.CompilerParams(collective_id=0, has_side_effects=True, vmem_limit_bytes=67043328),
            name="mlp_backward",
        )(x, dy, gate, up, w_gate, w_up, w_down)
        return tuple(res[:4])

    tok, col, row = P(("dp", "tp"), None), P("dp", "tp"), P("tp", None)
    wcol = P(None, "tp")
    return jax.shard_map(
        body, mesh=mesh, in_specs=(tok, tok, col, col, wcol, wcol, row), out_specs=(tok, col, col, tok), check_vma=False
    )
```

```python
import functools

import jax
import jax.numpy as jnp
from jax import lax
from jax.experimental import pallas as pl
from jax.experimental.pallas import tpu as pltpu
from jax.sharding import PartitionSpec as P

MESH = pl.DeviceIdType.MESH
BF16, F32 = jnp.bfloat16, jnp.float32
NT = (((1,), (1,)), ((), ()))
TN = (((0,), (0,)), ((), ()))


def act(gate, up):
    return jax.nn.gelu(gate) * up


def kernel(
    n, x_ref, dy_ref, gate_ref, up_ref, wg_ref, wu_ref, wd_ref,
    dx_ref, dwg_ref, dwu_ref, dwd_ref, dyg, xg, pbuf,
    wgu_v, dgu_v, hid_v, tile_v, gu_v, dh_v, psend, rsend, rrecv, acc_v, strip_v,
    ag_s, ag_r, p_s, p_r, q_s, q_r, w_sem, g_sem, t_sem, own_sem, st_sem, dx_sem,
):
    me = lax.axis_index("tp")
    core = lax.rem(me, 2)
    other = 1 - 2 * core
    right, left, far = lax.rem(me + 2, n), lax.rem(me + n - 2, n), lax.rem(me + 4, n)
    partner = me + other
    R, D = dy_ref.shape
    H = R // 2
    F = gate_ref.shape[1]
    T = n * R

    def rows(block, half=None):
        if half is None:
            return pl.ds(pl.multiple_of(block * R, R), R)
        return pl.ds(pl.multiple_of(block * R + half * H, H), H)

    def local(src, dst, sem):
        return pltpu.make_async_copy(src, dst, sem)

    def remote(src, dst, s, r, to):
        return pltpu.make_async_remote_copy(src_ref=src, dst_ref=dst, send_sem=s, recv_sem=r, device_id={"tp": to}, device_id_type=MESH)

    pieces = ((left, 0), (left, 1), (right, 1), (right, 0), (far, 0), (far, 1))
    own_sends = ((right, 0), (right, 1), (left, 1), (left, 0))
    own = (psend.at[0], x_ref)
    full = (dyg, xg)

    def ring_own(a, k):
        to, half = own_sends[k]
        return remote(own[a].at[pl.ds(half * H, H)], full[a].at[rows(me, half)], ag_s.at[a, k], ag_r.at[a, k], to)

    def ring_fwd(a, k):
        block, half, to = ((left, 0, right), (right, 1, left))[k - 4]
        ref = full[a].at[rows(block, half)]
        return remote(ref, ref, ag_s.at[a, k], ag_r.at[a, k], to)

    def ring_arrived(a, k):
        block, half = pieces[k]
        ref = full[a].at[rows(block, half)]
        remote(ref, ref, ag_s.at[a, k], ag_r.at[a, k], partner).wait_recv()

    def pair_own(a):
        return remote(own[a], full[a].at[rows(me)], ag_s.at[a, 6], ag_r.at[a, 6], partner)

    def pair_fwd(a, k):
        block, half = pieces[k]
        ref = full[a].at[rows(block, half)]
        return remote(ref, ref, ag_s.at[a, 7 + k], ag_r.at[a, 7 + k], partner)

    def pair_arrived(a, k):
        if k < 0:
            ref = full[a].at[rows(partner)]
            remote(ref, ref, ag_s.at[a, 6], ag_r.at[a, 6], partner).wait_recv()
        else:
            block, half = pieces[k]
            ref = full[a].at[rows(block + other, half)]
            remote(ref, ref, ag_s.at[a, 7 + k], ag_r.at[a, 7 + k], partner).wait_recv()

    wd_v = dwd_ref
    w_copies = (
        local(wd_ref, wd_v, w_sem.at[0]),
        local(wg_ref, wgu_v.at[:, pl.ds(0, F)], w_sem.at[1]),
        local(wu_ref, wgu_v.at[:, pl.ds(F, F)], w_sem.at[2]),
    )

    stage = [local(dy_ref.at[pl.ds(h * H, H)], psend.at[0, pl.ds(h * H, H)], dx_sem.at[h]) for h in range(2)]
    for c in stage:
        c.start()

    barrier = pltpu.get_barrier_semaphore()
    for to in (left, right, partner):
        pl.semaphore_signal(barrier, inc=1, device_id={"tp": to}, device_id_type=MESH)
    pl.semaphore_wait(barrier, 3)

    for c in stage:
        c.wait()
    for k in (0, 2, 1, 3):
        ring_own(0, k).start()
    pair_own(0).start()
    pair_own(1).start()

    def block_of(s):
        j = s // 2
        hop = j + j // 2 - 2 * (j // 3)
        return lax.rem(me + 2 * hop, n) + lax.rem(s, 2) * other

    def gate_load(s, slot):
        r = rows(block_of(s))
        return (
            local(gate_ref.at[r], gu_v.at[slot, 0], g_sem.at[slot, 0]),
            local(up_ref.at[r], gu_v.at[slot, 1], g_sem.at[slot, 1]),
        )

    def tile_load(s, slot):
        return local(dyg.at[rows(block_of(s))], tile_v.at[slot], t_sem.at[slot])

    w_copies[0].start()
    local(dy_ref, tile_v.at[0], t_sem.at[0]).start()
    for c in gate_load(0, 0):
        c.start()
    x_stage = local(x_ref, psend.at[1], own_sem.at[1])
    x_stage.start()
    w_copies[1].start()
    w_copies[2].start()
    x_stage.wait()
    stage = [local(psend.at[0], dyg.at[rows(me)], own_sem.at[0]), local(psend.at[1], xg.at[rows(me)], own_sem.at[1])]
    for c in stage:
        c.start()
    w_copies[0].wait()

    def step(s, _):
        slot, nxt = lax.rem(s, 2), lax.rem(s + 1, 2)
        r = rows(block_of(s))
        tile_load(s, slot).wait()
        for c in gate_load(s, slot):
            c.wait()
        dh_v[...] = lax.dot_general(tile_v[slot], wd_v[...], NT, preferred_element_type=F32)

        @pl.when(s == 0)
        def _():
            pair_arrived(0, -1)

        @pl.when(s == 1)
        def _():
            for k in (0, 2):
                ring_arrived(0, k)
            for k in (4, 5):
                ring_fwd(0, k).start()
            for k in (0, 2, 1, 3):
                ring_own(1, k).start()
            for k in (0, 2):
                pair_fwd(0, k).start()
            for k in (1, 3):
                ring_arrived(0, k)
                pair_fwd(0, k).start()

        @pl.when(s == 2)
        def _():
            for k in (2, 3):
                pair_arrived(0, k)

        @pl.when(s == 4)
        def _():
            for k in (0, 1):
                pair_arrived(0, k)

        @pl.when(s == 5)
        def _():
            for k in (4, 5):
                ring_arrived(0, k)
                pair_fwd(0, k).start()

        @pl.when(s == 6)
        def _():
            for k in (4, 5):
                pair_arrived(0, k)

        @pl.when(s < n - 1)
        def _():
            tile_load(s + 1, nxt).start()
            for c in gate_load(s + 1, nxt):
                c.start()

        def chunk(i, _):
            m = 16
            q = pl.ds(pl.multiple_of(i * m, m), m)
            o = pl.ds(pl.multiple_of(block_of(s) * R + i * m, m), m)
            hidden, back = jax.vjp(act, gu_v[slot, 0, q].astype(F32), gu_v[slot, 1, q].astype(F32))
            dg, du = back(dh_v[q])
            dgu_v[o, pl.ds(0, F)] = dg.astype(BF16)
            dgu_v[o, pl.ds(F, F)] = du.astype(BF16)
            hid_v[o] = hidden.astype(BF16)
            return 0

        lax.fori_loop(0, R // 16, chunk, 0)
        return 0

    lax.fori_loop(0, n, step, 0)
    for c in stage:
        c.wait()
    for c in w_copies[1:]:
        c.wait()

    NB = 512

    def dx_terms(row0, m, emit):
        def ntile(t, _):
            cols = pl.ds(pl.multiple_of(t * NB, NB), NB)
            emit(cols, lax.dot_general(dgu_v[pl.ds(row0, m)], wgu_v[cols], NT, preferred_element_type=F32))
            return 0

        lax.fori_loop(0, D // NB, ntile, 0)

    targets = (far, right, left, me)

    def p_copy(i):
        return remote(psend.at[i % 2], pbuf.at[i], p_s.at[i], p_r.at[i], partner)

    for k in range(4):
        ring_own(0, k).wait_send()
    pair_own(0).wait_send()
    for i, block in enumerate(targets):
        if i >= 2:
            p_copy(i - 2).wait_send()

        def emit(cols, v, i=i):
            psend[i % 2, :, cols] = v.astype(BF16)

        dx_terms(pl.multiple_of((block + other) * R, R), R, emit)
        p_copy(i).start()

    for k in (0, 2):
        ring_arrived(1, k)
    for k in (4, 5):
        ring_fwd(1, k).start()
    for k in (0, 2):
        pair_fwd(1, k).start()

    def p_load(i, half=None):
        if half is None:
            return local(pbuf.at[i], tile_v.at[i % 2], t_sem.at[i % 2])
        h = pl.ds(half * H, H)
        return local(pbuf.at[i, h], tile_v.at[i % 2, h], t_sem.at[i % 2])

    def p_fetch(i):
        p_copy(i).wait_recv()
        p_load(i).start()

    cuts = (0, H // 2, 3 * H // 4, 7 * H // 8, H)

    def q_src(q):
        return rsend.at[q] if q < 4 else psend.at[0, pl.ds((q - 4) * H, H)]

    def q_part(q, sub=None):
        lo, hi, k = (0, H, q) if sub is None else (cuts[sub], cuts[sub + 1], q + 2 * sub)
        h = pl.ds(lo, hi - lo)
        return remote(q_src(q).at[h], rrecv.at[q, h], q_s.at[k], q_r.at[k], (right, left)[q % 2])

    def q_parts(q):
        return [q_part(q)] if q < 4 else [q_part(q, sub) for sub in range(4)]

    def ring_sum(q, i, half, add=None):
        h = pl.ds(half * H, H)
        dst = q_src(q)

        def emit(cols, v):
            v = v + tile_v[i % 2, h, cols].astype(F32)
            if add is not None:
                v = v + rrecv[add, :, cols].astype(F32)
            dst[:, cols] = v.astype(BF16)

        dx_terms(pl.multiple_of(targets[i] * R + half * H, H), H, emit)
        if q < 4:
            q_part(q).start()

    p_fetch(0)
    p_fetch(1)
    p_load(0).wait()
    ring_sum(0, 0, 0)
    ring_sum(1, 0, 1)
    p_fetch(2)
    p_load(1).wait()
    ring_sum(2, 1, 1)
    p_fetch(3)
    p_load(2).wait()
    ring_sum(3, 2, 0)
    p_load(3).wait()

    def emit_own(cols, v):
        acc_v[:, cols] = v + tile_v[1, :, cols].astype(F32)

    dx_terms(pl.multiple_of(me * R, R), R, emit_own)

    for k in (1, 3):
        ring_arrived(1, k)
        pair_fwd(1, k).start()

    W = strip_v.shape[2]

    def strip_load(a, t, slot):
        return local(full[a].at[:, pl.ds(pl.multiple_of(t * W, W), W)], strip_v.at[slot], st_sem.at[slot])

    def strips(a, lo, hi, work):
        strip_load(a, lo, lo % 2).start()

        def one(t, _):
            slot = lax.rem(t, 2)
            strip_load(a, t, slot).wait()

            @pl.when(t + 1 < hi)
            def _():
                strip_load(a, t + 1, 1 - slot).start()

            work(slot, pl.ds(pl.multiple_of(t * W, W), W))
            return 0

        lax.fori_loop(lo, hi, one, 0)

    def down_work(slot, part):
        v = lax.dot_general(strip_v[slot], hid_v[...], TN, preferred_element_type=F32)
        dwd_ref[:, part] = v.T.astype(BF16)

    def in_work(slot, part):
        v = lax.dot_general(strip_v[slot], dgu_v[...], TN, preferred_element_type=F32)
        dwg_ref[part] = v[:, :F].astype(BF16)
        dwu_ref[part] = v[:, F:].astype(BF16)

    S = D // W
    strips(0, 0, S, down_work)

    for k in (4, 5):
        ring_arrived(1, k)
        pair_fwd(1, k).start()
    for k in (-1, 0, 1, 2, 3, 4, 5):
        pair_arrived(1, k)

    strips(1, 0, S // 2, in_work)

    for i, half in ((1, 0), (2, 1)):
        p_load(i, half).start()
    for c in q_parts(0) + q_parts(1):
        c.wait_recv()
    for i, half in ((1, 0), (2, 1)):
        p_load(i, half).wait()
    for i in (2, 3):
        p_copy(i).wait_send()
    ring_sum(4, 1, 0, add=0)
    ring_sum(5, 2, 1, add=1)
    for sub in range(4):
        for q in (4, 5):
            q_part(q, sub).start()

    strips(1, S // 2, S, in_work)

    for q in (2, 3):
        q_part(q).wait_recv()
    for sub in range(4):
        for q, first, base in ((4, 3, 0), (5, 2, H)):
            q_part(q, sub).wait_recv()

            def put(i, _, q=q, first=first, base=base, lo=cuts[sub]):
                h = pl.ds(pl.multiple_of(lo + i * 16, 16), 16)
                r = pl.ds(pl.multiple_of(base + lo + i * 16, 16), 16)
                v = acc_v[r] + rrecv[first, h].astype(F32) + rrecv[q, h].astype(F32)
                dx_ref[r] = v.astype(BF16)
                return 0

            lax.fori_loop(0, (cuts[sub + 1] - cuts[sub]) // 16, put, 0)

    for k in range(4):
        ring_own(1, k).wait_send()
    pair_own(1).wait_send()
    for a in range(2):
        for k in (4, 5):
            ring_fwd(a, k).wait_send()
        for k in range(6):
            pair_fwd(a, k).wait_send()
    for q in range(6):
        for c in q_parts(q):
            c.wait_send()


def write_out(*refs):
    k = len(refs) // 2
    copies = [pltpu.make_async_copy(refs[i], refs[k + i], refs[-1].at[i]) for i in range(k)]
    for c in copies:
        c.start()
    for c in copies:
        c.wait()


def solution(mesh):
    n = mesh.shape["tp"]

    def body(x, dy, gate, up, w_gate, w_up, w_down):
        R, D = x.shape
        T, F = gate.shape
        H = R // 2
        W = 256
        out = lambda *s: jax.ShapeDtypeStruct(s, BF16)
        results = ((R, D), (D, F), (D, F), (F, D))
        vmem_spec = pl.BlockSpec(memory_space=pltpu.VMEM)
        any_spec = pl.BlockSpec(memory_space=pl.ANY)
        dma = pltpu.SemaphoreType.DMA
        res = pl.pallas_call(
            functools.partial(kernel, n),
            out_shape=[pltpu.VMEM(s, BF16) for s in results] + [out(T, D), out(T, D), out(4, R, D)],
            in_specs=[any_spec] * 7,
            out_specs=[vmem_spec] * 4 + [any_spec] * 3,
            scratch_shapes=[
                pltpu.VMEM((D, 2 * F), BF16),
                pltpu.VMEM((T, 2 * F), BF16),
                pltpu.VMEM((T, F), BF16),
                pltpu.VMEM((2, R, D), BF16),
                pltpu.VMEM((2, 2, R, F), BF16),
                pltpu.VMEM((R, F), F32),
                pltpu.VMEM((2, R, D), BF16),
                pltpu.VMEM((4, H, D), BF16),
                pltpu.VMEM((6, H, D), BF16),
                pltpu.VMEM((R, D), F32),
                pltpu.VMEM((2, T, W), BF16),
                dma((2, 13)), dma((2, 13)),
                dma((4,)), dma((4,)),
                dma((12,)), dma((12,)),
                dma((3,)), dma((2, 2)), dma((2,)), dma((2,)),
                dma((2,)), dma((2,)),
            ],
            compiler_params=pltpu.CompilerParams(collective_id=0, has_side_effects=True, vmem_limit_bytes=217 * 2**18),
            name="mlp_backward",
        )(x, dy, gate, up, w_gate, w_up, w_down)
        return tuple(
            pl.pallas_call(
                write_out,
                out_shape=[out(*s) for s in results],
                in_specs=[vmem_spec] * 4,
                out_specs=[any_spec] * 4,
                scratch_shapes=[dma((4,))],
                compiler_params=pltpu.CompilerParams(vmem_limit_bytes=2**18),
                name="write_results",
            )(*(pltpu.with_memory_space_constraint(r, pltpu.VMEM) for r in res[:4]))
        )

    tok, col, row = P(("dp", "tp"), None), P("dp", "tp"), P("tp", None)
    wcol = P(None, "tp")
    return jax.shard_map(
        body, mesh=mesh, in_specs=(tok, tok, col, col, wcol, wcol, row), out_specs=(tok, col, col, tok), check_vma=False
    )
```

```python
import functools

import jax
import jax.numpy as jnp
from jax import lax
from jax.experimental import pallas as pl
from jax.experimental.pallas import tpu as pltpu
from jax.sharding import PartitionSpec as P

MESH = pl.DeviceIdType.MESH
BF16, F32 = jnp.bfloat16, jnp.float32
NT = (((1,), (1,)), ((), ()))
TN = (((0,), (0,)), ((), ()))


def act(gate, up):
    return jax.nn.gelu(gate) * up


def kernel(
    n, x_ref, dy_ref, gate_ref, up_ref, wg_ref, wu_ref, wd_ref,
    dx_ref, dwg_ref, dwu_ref, dwd_ref, dyg, xg, pbuf,
    wgu_v, dgu_v, hid_v, tile_v, gu_v, dh_v, psend, rsend, rrecv, acc_v, strip_v,
    ag_s, ag_r, p_s, p_r, q_s, q_r, w_sem, g_sem, t_sem, own_sem, st_sem,
):
    me = lax.axis_index("tp")
    core = lax.rem(me, 2)
    other = 1 - 2 * core
    right, left, far = lax.rem(me + 2, n), lax.rem(me + n - 2, n), lax.rem(me + 4, n)
    partner = me + other
    R, D = dy_ref.shape
    H = R // 2
    F = gate_ref.shape[1]
    T = n * R

    def rows(block, half=None):
        if half is None:
            return pl.ds(pl.multiple_of(block * R, R), R)
        return pl.ds(pl.multiple_of(block * R + half * H, H), H)

    def local(src, dst, sem):
        return pltpu.make_async_copy(src, dst, sem)

    def remote(src, dst, s, r, to):
        return pltpu.make_async_remote_copy(src_ref=src, dst_ref=dst, send_sem=s, recv_sem=r, device_id={"tp": to}, device_id_type=MESH)

    pieces = ((left, 0), (left, 1), (right, 1), (right, 0), (far, 0), (far, 1))
    own_sends = ((right, 0), (right, 1), (left, 1), (left, 0))
    own = (dy_ref, x_ref)
    full = (dyg, xg)

    def ring_own(a, k):
        to, half = own_sends[k]
        return remote(own[a].at[pl.ds(half * H, H)], full[a].at[rows(me, half)], ag_s.at[a, k], ag_r.at[a, k], to)

    def ring_fwd(a, k):
        block, half, to = ((left, 0, right), (right, 1, left))[k - 4]
        ref = full[a].at[rows(block, half)]
        return remote(ref, ref, ag_s.at[a, k], ag_r.at[a, k], to)

    def ring_arrived(a, k):
        block, half = pieces[k]
        ref = full[a].at[rows(block, half)]
        remote(ref, ref, ag_s.at[a, k], ag_r.at[a, k], partner).wait_recv()

    def pair_own(a):
        return remote(own[a], full[a].at[rows(me)], ag_s.at[a, 6], ag_r.at[a, 6], partner)

    def pair_fwd(a, k):
        block, half = pieces[k]
        ref = full[a].at[rows(block, half)]
        return remote(ref, ref, ag_s.at[a, 7 + k], ag_r.at[a, 7 + k], partner)

    def pair_arrived(a, k):
        if k < 0:
            ref = full[a].at[rows(partner)]
            remote(ref, ref, ag_s.at[a, 6], ag_r.at[a, 6], partner).wait_recv()
        else:
            block, half = pieces[k]
            ref = full[a].at[rows(block + other, half)]
            remote(ref, ref, ag_s.at[a, 7 + k], ag_r.at[a, 7 + k], partner).wait_recv()

    wd_v = dwd_ref
    w_copies = (
        local(wd_ref, wd_v, w_sem.at[0]),
        local(wg_ref, wgu_v.at[:, pl.ds(0, F)], w_sem.at[1]),
        local(wu_ref, wgu_v.at[:, pl.ds(F, F)], w_sem.at[2]),
    )

    barrier = pltpu.get_barrier_semaphore()
    for to in (left, right, partner):
        pl.semaphore_signal(barrier, inc=1, device_id={"tp": to}, device_id_type=MESH)
    pl.semaphore_wait(barrier, 3)

    for k in (0, 2, 1, 3):
        ring_own(0, k).start()
    pair_own(0).start()
    pair_own(1).start()

    def block_of(s):
        j = s // 2
        hop = j + j // 2 - 2 * (j // 3)
        return lax.rem(me + 2 * hop, n) + lax.rem(s, 2) * other

    def gate_load(s, slot):
        r = rows(block_of(s))
        return (
            local(gate_ref.at[r], gu_v.at[slot, 0], g_sem.at[slot, 0]),
            local(up_ref.at[r], gu_v.at[slot, 1], g_sem.at[slot, 1]),
        )

    def tile_load(s, slot):
        return local(dyg.at[rows(block_of(s))], tile_v.at[slot], t_sem.at[slot])

    w_copies[0].start()
    local(dy_ref, tile_v.at[0], t_sem.at[0]).start()
    for c in gate_load(0, 0):
        c.start()
    stage = [local(dy_ref, psend.at[0], own_sem.at[0]), local(x_ref, psend.at[1], own_sem.at[1])]
    for c in stage:
        c.start()
    w_copies[1].start()
    w_copies[2].start()
    for c in stage:
        c.wait()
    stage = [local(psend.at[0], dyg.at[rows(me)], own_sem.at[0]), local(psend.at[1], xg.at[rows(me)], own_sem.at[1])]
    for c in stage:
        c.start()
    w_copies[0].wait()

    def step(s, _):
        slot, nxt = lax.rem(s, 2), lax.rem(s + 1, 2)
        r = rows(block_of(s))
        tile_load(s, slot).wait()
        for c in gate_load(s, slot):
            c.wait()
        dh_v[...] = lax.dot_general(tile_v[slot], wd_v[...], NT, preferred_element_type=F32)

        @pl.when(s == 0)
        def _():
            pair_arrived(0, -1)

        @pl.when(s == 1)
        def _():
            for k in (0, 2):
                ring_arrived(0, k)
            for k in (4, 5):
                ring_fwd(0, k).start()
            for k in (0, 2, 1, 3):
                ring_own(1, k).start()
            for k in (0, 2):
                pair_fwd(0, k).start()
            for k in (1, 3):
                ring_arrived(0, k)
                pair_fwd(0, k).start()

        @pl.when(s == 2)
        def _():
            for k in (2, 3):
                pair_arrived(0, k)

        @pl.when(s == 4)
        def _():
            for k in (0, 1):
                pair_arrived(0, k)

        @pl.when(s == 5)
        def _():
            for k in (4, 5):
                ring_arrived(0, k)
                pair_fwd(0, k).start()

        @pl.when(s == 6)
        def _():
            for k in (4, 5):
                pair_arrived(0, k)

        @pl.when(s < n - 1)
        def _():
            tile_load(s + 1, nxt).start()
            for c in gate_load(s + 1, nxt):
                c.start()

        def chunk(i, _):
            m = 16
            q = pl.ds(pl.multiple_of(i * m, m), m)
            o = pl.ds(pl.multiple_of(block_of(s) * R + i * m, m), m)
            hidden, back = jax.vjp(act, gu_v[slot, 0, q].astype(F32), gu_v[slot, 1, q].astype(F32))
            dg, du = back(dh_v[q])
            dgu_v[o, pl.ds(0, F)] = dg.astype(BF16)
            dgu_v[o, pl.ds(F, F)] = du.astype(BF16)
            hid_v[o] = hidden.astype(BF16)
            return 0

        lax.fori_loop(0, R // 16, chunk, 0)
        return 0

    lax.fori_loop(0, n, step, 0)
    for c in stage:
        c.wait()
    for c in w_copies[1:]:
        c.wait()

    NB = 512

    def dx_terms(row0, m, emit):
        def ntile(t, _):
            cols = pl.ds(pl.multiple_of(t * NB, NB), NB)
            emit(cols, lax.dot_general(dgu_v[pl.ds(row0, m)], wgu_v[cols], NT, preferred_element_type=F32))
            return 0

        lax.fori_loop(0, D // NB, ntile, 0)

    targets = (far, right, left, me)

    def p_copy(i):
        return remote(psend.at[i % 2], pbuf.at[i], p_s.at[i], p_r.at[i], partner)

    for i, block in enumerate(targets):
        if i >= 2:
            p_copy(i - 2).wait_send()

        def emit(cols, v, i=i):
            psend[i % 2, :, cols] = v.astype(BF16)

        dx_terms(pl.multiple_of((block + other) * R, R), R, emit)
        p_copy(i).start()

    for k in (0, 2):
        ring_arrived(1, k)
    for k in (4, 5):
        ring_fwd(1, k).start()
    for k in (0, 2):
        pair_fwd(1, k).start()

    def p_load(i, half=None):
        if half is None:
            return local(pbuf.at[i], tile_v.at[i % 2], t_sem.at[i % 2])
        h = pl.ds(half * H, H)
        return local(pbuf.at[i, h], tile_v.at[i % 2, h], t_sem.at[i % 2])

    def p_fetch(i):
        p_copy(i).wait_recv()
        p_load(i).start()

    C = 8
    PIECE = H // C

    def q_src(q):
        return rsend.at[q] if q < 4 else psend.at[0, pl.ds((q - 4) * H, H)]

    def q_part(q, sub=None):
        h, k = (pl.ds(0, H), q) if sub is None else (pl.ds(pl.multiple_of(sub * PIECE, PIECE), PIECE), q + 2 * sub)
        return remote(q_src(q).at[h], rrecv.at[q, h], q_s.at[k], q_r.at[k], (right, left)[q % 2])

    def q_parts(q):
        return [q_part(q)] if q < 4 else [q_part(q, sub) for sub in range(C)]

    def ring_sum(q, i, half, add=None):
        h = pl.ds(half * H, H)
        dst = q_src(q)

        def emit(cols, v):
            v = v + tile_v[i % 2, h, cols].astype(F32)
            if add is not None:
                v = v + rrecv[add, :, cols].astype(F32)
            dst[:, cols] = v.astype(BF16)

        dx_terms(pl.multiple_of(targets[i] * R + half * H, H), H, emit)
        if q < 4:
            q_part(q).start()

    p_fetch(0)
    p_fetch(1)
    p_load(0).wait()
    ring_sum(0, 0, 0)
    ring_sum(1, 0, 1)
    p_fetch(2)
    p_load(1).wait()
    ring_sum(2, 1, 1)
    p_fetch(3)
    p_load(2).wait()
    ring_sum(3, 2, 0)
    p_load(3).wait()

    def emit_own(cols, v):
        acc_v[:, cols] = v + tile_v[1, :, cols].astype(F32)

    dx_terms(pl.multiple_of(me * R, R), R, emit_own)

    for k in (1, 3):
        ring_arrived(1, k)
        pair_fwd(1, k).start()

    W = strip_v.shape[2]

    def strip_load(a, t, slot):
        return local(full[a].at[:, pl.ds(pl.multiple_of(t * W, W), W)], strip_v.at[slot], st_sem.at[slot])

    def strips(a, lo, hi, work):
        strip_load(a, lo, lo % 2).start()

        def one(t, _):
            slot = lax.rem(t, 2)
            strip_load(a, t, slot).wait()

            @pl.when(t + 1 < hi)
            def _():
                strip_load(a, t + 1, 1 - slot).start()

            work(slot, pl.ds(pl.multiple_of(t * W, W), W))
            return 0

        lax.fori_loop(lo, hi, one, 0)

    def down_work(slot, part):
        v = lax.dot_general(strip_v[slot], hid_v[...], TN, preferred_element_type=F32)
        dwd_ref[:, part] = v.T.astype(BF16)

    def in_work(slot, part):
        v = lax.dot_general(strip_v[slot], dgu_v[...], TN, preferred_element_type=F32)
        dwg_ref[part] = v[:, :F].astype(BF16)
        dwu_ref[part] = v[:, F:].astype(BF16)

    S = D // W
    strips(0, 0, S, down_work)

    for k in (4, 5):
        ring_arrived(1, k)
        pair_fwd(1, k).start()
    for k in (-1, 0, 1, 2, 3, 4, 5):
        pair_arrived(1, k)

    strips(1, 0, S // 2, in_work)

    for i, half in ((1, 0), (2, 1)):
        p_load(i, half).start()
    for c in q_parts(0) + q_parts(1):
        c.wait_recv()
    for i, half in ((1, 0), (2, 1)):
        p_load(i, half).wait()
    for i in (2, 3):
        p_copy(i).wait_send()
    ring_sum(4, 1, 0, add=0)
    ring_sum(5, 2, 1, add=1)
    for sub in range(C):
        for q in (4, 5):
            q_part(q, sub).start()

    strips(1, S // 2, S, in_work)

    for a in range(2):
        for k in range(4):
            ring_own(a, k).wait_send()
        pair_own(a).wait_send()
        for k in (4, 5):
            ring_fwd(a, k).wait_send()
        for k in range(6):
            pair_fwd(a, k).wait_send()
    for q in range(4):
        q_part(q).wait_send()
    for q in (2, 3):
        q_part(q).wait_recv()

    def finish(sub, _):
        for q, first, base in ((4, 3, 0), (5, 2, H)):
            q_part(q, sub).wait_recv()

            def put(i, _):
                h = pl.ds(pl.multiple_of(sub * PIECE + i * 16, 16), 16)
                r = pl.ds(pl.multiple_of(base + sub * PIECE + i * 16, 16), 16)
                v = acc_v[r] + rrecv[first, h].astype(F32) + rrecv[q, h].astype(F32)
                dx_ref[r] = v.astype(BF16)
                return 0

            lax.fori_loop(0, PIECE // 16, put, 0)
        for q in (4, 5):
            q_part(q, sub).wait_send()
        return 0

    lax.fori_loop(0, C, finish, 0)


def write_out(*refs):
    k = len(refs) // 2
    copies = [pltpu.make_async_copy(refs[i], refs[k + i], refs[-1].at[i]) for i in range(k)]
    for c in copies:
        c.start()
    for c in copies:
        c.wait()


def solution(mesh):
    n = mesh.shape["tp"]

    def body(x, dy, gate, up, w_gate, w_up, w_down):
        R, D = x.shape
        T, F = gate.shape
        H = R // 2
        W = 256
        out = lambda *s: jax.ShapeDtypeStruct(s, BF16)
        results = ((R, D), (D, F), (D, F), (F, D))
        vmem_spec = pl.BlockSpec(memory_space=pltpu.VMEM)
        any_spec = pl.BlockSpec(memory_space=pl.ANY)
        dma = pltpu.SemaphoreType.DMA
        res = pl.pallas_call(
            functools.partial(kernel, n),
            out_shape=[pltpu.VMEM(s, BF16) for s in results] + [out(T, D), out(T, D), out(4, R, D)],
            in_specs=[any_spec] * 7,
            out_specs=[vmem_spec] * 4 + [any_spec] * 3,
            scratch_shapes=[
                pltpu.VMEM((D, 2 * F), BF16),
                pltpu.VMEM((T, 2 * F), BF16),
                pltpu.VMEM((T, F), BF16),
                pltpu.VMEM((2, R, D), BF16),
                pltpu.VMEM((2, 2, R, F), BF16),
                pltpu.VMEM((R, F), F32),
                pltpu.VMEM((2, R, D), BF16),
                pltpu.VMEM((4, H, D), BF16),
                pltpu.VMEM((6, H, D), BF16),
                pltpu.VMEM((R, D), F32),
                pltpu.VMEM((2, T, W), BF16),
                dma((2, 13)), dma((2, 13)),
                dma((4,)), dma((4,)),
                dma((20,)), dma((20,)),
                dma((3,)), dma((2, 2)), dma((2,)), dma((2,)),
                dma((2,)),
            ],
            compiler_params=pltpu.CompilerParams(collective_id=0, has_side_effects=True, vmem_limit_bytes=217 * 2**18),
            name="mlp_backward",
        )(x, dy, gate, up, w_gate, w_up, w_down)
        return tuple(
            pl.pallas_call(
                write_out,
                out_shape=[out(*s) for s in results],
                in_specs=[vmem_spec] * 4,
                out_specs=[any_spec] * 4,
                scratch_shapes=[dma((4,))],
                compiler_params=pltpu.CompilerParams(vmem_limit_bytes=2**18),
                name="write_results",
            )(*(pltpu.with_memory_space_constraint(r, pltpu.VMEM) for r in res[:4]))
        )

    tok, col, row = P(("dp", "tp"), None), P("dp", "tp"), P("tp", None)
    wcol = P(None, "tp")
    return jax.shard_map(
        body, mesh=mesh, in_specs=(tok, tok, col, col, wcol, wcol, row), out_specs=(tok, col, col, tok), check_vma=False
    )
```

```python
import functools

import jax
import jax.numpy as jnp
from jax import lax
from jax.experimental import pallas as pl
from jax.experimental.pallas import tpu as pltpu
from jax.sharding import PartitionSpec as P

MESH = pl.DeviceIdType.MESH
BF16, F32 = jnp.bfloat16, jnp.float32
NT = (((1,), (1,)), ((), ()))
TN = (((0,), (0,)), ((), ()))
C = 8


def act(gate, up):
    return jax.nn.gelu(gate) * up


def kernel(
    n, early, x_ref, dy_ref, gate_ref, up_ref, wg_ref, wu_ref, wd_ref,
    dwg_ref, dwu_ref, dwd_ref, acc_v, last_v, dyg, xg, pbuf,
    wgu_v, dgu_v, hid_v, tile_v, gu_v, dh_v, psend, rsend, rrecv, strip_v,
    ag_s, ag_r, p_s, p_r, q_s, q_r, w_sem, g_sem, t_sem, own_sem, st_sem,
):
    me = lax.axis_index("tp")
    core = lax.rem(me, 2)
    other = 1 - 2 * core
    right, left, far = lax.rem(me + 2, n), lax.rem(me + n - 2, n), lax.rem(me + 4, n)
    partner = me + other
    R, D = dy_ref.shape
    H = R // 2
    F = gate_ref.shape[1]
    T = n * R

    def rows(block, half=None):
        if half is None:
            return pl.ds(pl.multiple_of(block * R, R), R)
        return pl.ds(pl.multiple_of(block * R + half * H, H), H)

    def local(src, dst, sem):
        return pltpu.make_async_copy(src, dst, sem)

    def remote(src, dst, s, r, to):
        return pltpu.make_async_remote_copy(src_ref=src, dst_ref=dst, send_sem=s, recv_sem=r, device_id={"tp": to}, device_id_type=MESH)

    pieces = ((left, 0), (left, 1), (right, 1), (right, 0), (far, 0), (far, 1))
    own_sends = ((right, 0), (right, 1), (left, 1), (left, 0))
    own = (dy_ref, x_ref)
    full = (dyg, xg)

    def ring_own(a, k):
        to, half = own_sends[k]
        return remote(own[a].at[pl.ds(half * H, H)], full[a].at[rows(me, half)], ag_s.at[a, k], ag_r.at[a, k], to)

    def ring_fwd(a, k):
        block, half, to = ((left, 0, right), (right, 1, left))[k - 4]
        ref = full[a].at[rows(block, half)]
        return remote(ref, ref, ag_s.at[a, k], ag_r.at[a, k], to)

    def ring_arrived(a, k):
        block, half = pieces[k]
        ref = full[a].at[rows(block, half)]
        remote(ref, ref, ag_s.at[a, k], ag_r.at[a, k], partner).wait_recv()

    def pair_own(a):
        return remote(own[a], full[a].at[rows(me)], ag_s.at[a, 6], ag_r.at[a, 6], partner)

    def pair_fwd(a, k):
        block, half = pieces[k]
        ref = full[a].at[rows(block, half)]
        return remote(ref, ref, ag_s.at[a, 7 + k], ag_r.at[a, 7 + k], partner)

    def pair_arrived(a, k):
        if k < 0:
            ref = full[a].at[rows(partner)]
            remote(ref, ref, ag_s.at[a, 6], ag_r.at[a, 6], partner).wait_recv()
        else:
            block, half = pieces[k]
            ref = full[a].at[rows(block + other, half)]
            remote(ref, ref, ag_s.at[a, 7 + k], ag_r.at[a, 7 + k], partner).wait_recv()

    wd_v = dwd_ref
    w_copies = (
        local(wd_ref, wd_v, w_sem.at[0]),
        local(wg_ref, wgu_v.at[:, pl.ds(0, F)], w_sem.at[1]),
        local(wu_ref, wgu_v.at[:, pl.ds(F, F)], w_sem.at[2]),
    )

    barrier = pltpu.get_barrier_semaphore()
    for to in (left, right, partner):
        pl.semaphore_signal(barrier, inc=1, device_id={"tp": to}, device_id_type=MESH)
    pl.semaphore_wait(barrier, 3)

    for k in (0, 2, 1, 3):
        ring_own(0, k).start()
    pair_own(0).start()
    pair_own(1).start()

    def block_of(s):
        j = s // 2
        hop = j + j // 2 - 2 * (j // 3)
        return lax.rem(me + 2 * hop, n) + lax.rem(s, 2) * other

    def gate_load(s, slot):
        r = rows(block_of(s))
        return (
            local(gate_ref.at[r], gu_v.at[slot, 0], g_sem.at[slot, 0]),
            local(up_ref.at[r], gu_v.at[slot, 1], g_sem.at[slot, 1]),
        )

    def tile_load(s, slot):
        return local(dyg.at[rows(block_of(s))], tile_v.at[slot], t_sem.at[slot])

    w_copies[0].start()
    local(dy_ref, tile_v.at[0], t_sem.at[0]).start()
    for c in gate_load(0, 0):
        c.start()
    stage = [local(dy_ref, psend.at[0], own_sem.at[0]), local(x_ref, psend.at[1], own_sem.at[1])]
    for c in stage:
        c.start()
    w_copies[1].start()
    w_copies[2].start()
    for c in stage:
        c.wait()
    stage = [local(psend.at[0], dyg.at[rows(me)], own_sem.at[0]), local(psend.at[1], xg.at[rows(me)], own_sem.at[1])]
    for c in stage:
        c.start()
    w_copies[0].wait()

    def step(s, _):
        slot, nxt = lax.rem(s, 2), lax.rem(s + 1, 2)
        r = rows(block_of(s))
        tile_load(s, slot).wait()
        for c in gate_load(s, slot):
            c.wait()
        dh_v[...] = lax.dot_general(tile_v[slot], wd_v[...], NT, preferred_element_type=F32)

        @pl.when(s == 0)
        def _():
            pair_arrived(0, -1)

        @pl.when(s == 1)
        def _():
            for k in (0, 2):
                ring_arrived(0, k)
            for k in (4, 5):
                ring_fwd(0, k).start()
            for k in (0, 2, 1, 3):
                ring_own(1, k).start()
            for k in (0, 2):
                pair_fwd(0, k).start()
            for k in (1, 3):
                ring_arrived(0, k)
                pair_fwd(0, k).start()

        @pl.when(s == 2)
        def _():
            for k in (2, 3):
                pair_arrived(0, k)

        @pl.when(s == 4)
        def _():
            for k in (0, 1):
                pair_arrived(0, k)

        @pl.when(s == 5)
        def _():
            for k in (4, 5):
                ring_arrived(0, k)
                pair_fwd(0, k).start()

        @pl.when(s == 6)
        def _():
            for k in (4, 5):
                pair_arrived(0, k)

        @pl.when(s < n - 1)
        def _():
            tile_load(s + 1, nxt).start()
            for c in gate_load(s + 1, nxt):
                c.start()

        def chunk(i, _):
            m = 16
            q = pl.ds(pl.multiple_of(i * m, m), m)
            o = pl.ds(pl.multiple_of(block_of(s) * R + i * m, m), m)
            hidden, back = jax.vjp(act, gu_v[slot, 0, q].astype(F32), gu_v[slot, 1, q].astype(F32))
            dg, du = back(dh_v[q])
            dgu_v[o, pl.ds(0, F)] = dg.astype(BF16)
            dgu_v[o, pl.ds(F, F)] = du.astype(BF16)
            hid_v[o] = hidden.astype(BF16)
            return 0

        lax.fori_loop(0, R // 16, chunk, 0)
        return 0

    lax.fori_loop(0, n, step, 0)
    for c in stage:
        c.wait()
    for c in w_copies[1:]:
        c.wait()

    NB = 512

    def dx_terms(row0, m, emit):
        def ntile(t, _):
            cols = pl.ds(pl.multiple_of(t * NB, NB), NB)
            emit(cols, lax.dot_general(dgu_v[pl.ds(row0, m)], wgu_v[cols], NT, preferred_element_type=F32))
            return 0

        lax.fori_loop(0, D // NB, ntile, 0)

    targets = (far, right, left, me)

    def p_copy(i):
        return remote(psend.at[i % 2], pbuf.at[i], p_s.at[i], p_r.at[i], partner)

    for i, block in enumerate(targets):
        if i >= 2:
            p_copy(i - 2).wait_send()

        def emit(cols, v, i=i):
            psend[i % 2, :, cols] = v.astype(BF16)

        dx_terms(pl.multiple_of((block + other) * R, R), R, emit)
        p_copy(i).start()

    for k in (0, 2):
        ring_arrived(1, k)
    for k in (4, 5):
        ring_fwd(1, k).start()
    for k in (0, 2):
        pair_fwd(1, k).start()

    def p_load(i, half=None):
        if half is None:
            return local(pbuf.at[i], tile_v.at[i % 2], t_sem.at[i % 2])
        h = pl.ds(half * H, H)
        return local(pbuf.at[i, h], tile_v.at[i % 2, h], t_sem.at[i % 2])

    def p_fetch(i):
        p_copy(i).wait_recv()
        p_load(i).start()

    PIECE = H // C

    def q_src(q):
        return rsend.at[q] if q < 4 else last_v.at[q - 4]

    def q_part(q, sub=None):
        h, k = (pl.ds(0, H), q) if sub is None else (pl.ds(pl.multiple_of(sub * PIECE, PIECE), PIECE), q + 2 * sub)
        return remote(q_src(q).at[h], rrecv.at[q, h], q_s.at[k], q_r.at[k], (right, left)[q % 2])

    def q_parts(q):
        return [q_part(q)] if q < 4 else [q_part(q, sub) for sub in range(C)]

    def ring_sum(q, i, half, add=None):
        h = pl.ds(half * H, H)
        dst = q_src(q)

        def emit(cols, v):
            v = v + tile_v[i % 2, h, cols].astype(F32)
            if add is not None:
                v = v + rrecv[add, :, cols].astype(F32)
            dst[:, cols] = v.astype(BF16)

        dx_terms(pl.multiple_of(targets[i] * R + half * H, H), H, emit)
        if q < 4:
            q_part(q).start()

    p_fetch(0)
    p_fetch(1)
    p_load(0).wait()
    ring_sum(0, 0, 0)
    ring_sum(1, 0, 1)
    p_fetch(2)
    p_load(1).wait()
    ring_sum(2, 1, 1)
    p_fetch(3)
    p_load(2).wait()
    ring_sum(3, 2, 0)
    p_load(3).wait()

    def emit_own(cols, v):
        acc_v[:, cols] = v + tile_v[1, :, cols].astype(F32)

    dx_terms(pl.multiple_of(me * R, R), R, emit_own)

    for k in (1, 3):
        ring_arrived(1, k)
        pair_fwd(1, k).start()

    W = strip_v.shape[2]

    def strip_load(a, t, slot):
        return local(full[a].at[:, pl.ds(pl.multiple_of(t * W, W), W)], strip_v.at[slot], st_sem.at[slot])

    def strips(a, lo, hi, work):
        strip_load(a, lo, lo % 2).start()

        def one(t, _):
            slot = lax.rem(t, 2)
            strip_load(a, t, slot).wait()

            @pl.when(t + 1 < hi)
            def _():
                strip_load(a, t + 1, 1 - slot).start()

            work(slot, pl.ds(pl.multiple_of(t * W, W), W))
            return 0

        lax.fori_loop(lo, hi, one, 0)

    def down_work(slot, part):
        v = lax.dot_general(strip_v[slot], hid_v[...], TN, preferred_element_type=F32)
        dwd_ref[:, part] = v.T.astype(BF16)

    def in_work(slot, part):
        v = lax.dot_general(strip_v[slot], dgu_v[...], TN, preferred_element_type=F32)
        dwg_ref[part] = v[:, :F].astype(BF16)
        dwu_ref[part] = v[:, F:].astype(BF16)

    S = D // W
    strips(0, 0, S, down_work)

    for k in (4, 5):
        ring_arrived(1, k)
        pair_fwd(1, k).start()
    for k in (-1, 0, 1, 2, 3, 4, 5):
        pair_arrived(1, k)

    strips(1, 0, S // 2, in_work)

    for i, half in ((1, 0), (2, 1)):
        p_load(i, half).start()
    for c in q_parts(0) + q_parts(1):
        c.wait_recv()
    for i, half in ((1, 0), (2, 1)):
        p_load(i, half).wait()
    for i in (2, 3):
        p_copy(i).wait_send()
    ring_sum(4, 1, 0, add=0)
    ring_sum(5, 2, 1, add=1)

    @pl.when(core == 1)
    def _():
        for sub in range(early):
            for q in (4, 5):
                q_part(q, sub).start()


    strips(1, S // 2, S, in_work)

    for a in range(2):
        for k in range(4):
            ring_own(a, k).wait_send()
        pair_own(a).wait_send()
        for k in (4, 5):
            ring_fwd(a, k).wait_send()
        for k in range(6):
            pair_fwd(a, k).wait_send()
    for q in range(4):
        q_part(q).wait_send()
    for q in (2, 3):
        q_part(q).wait_recv()

    def settle(i, _):
        h = pl.ds(pl.multiple_of(i * 16, 16), 16)
        for q, base in ((3, 0), (2, H)):
            r = pl.ds(pl.multiple_of(base + i * 16, 16), 16)
            acc_v[r] = acc_v[r] + rrecv[q, h].astype(F32)
        return 0

    lax.fori_loop(0, H // 16, settle, 0)

    @pl.when(core == 1)
    def _():
        def finish(sub, _):
            for q, base in ((4, 0), (5, H)):
                q_part(q, sub).wait_recv()

                def put(i, _):
                    h = pl.ds(pl.multiple_of(sub * PIECE + i * 16, 16), 16)
                    r = pl.ds(pl.multiple_of(base + sub * PIECE + i * 16, 16), 16)
                    acc_v[r] = acc_v[r] + rrecv[q, h].astype(F32)
                    return 0

                lax.fori_loop(0, PIECE // 16, put, 0)
            for q in (4, 5):
                q_part(q, sub).wait_send()
            return 0

        lax.fori_loop(0, early, finish, 0)


def last_hop(n, early, acc_v, last_v, after_ref, dx_ref, recv_v, s_sem, r_sem):
    me = lax.axis_index("tp")
    core = lax.rem(me, 2)
    to = (lax.rem(me + 2, n), lax.rem(me + n - 2, n))
    H = acc_v.shape[0] // 2
    PIECE = H // C

    barrier = pltpu.get_barrier_semaphore()
    for t in to:
        pl.semaphore_signal(barrier, inc=1, device_id={"tp": t}, device_id_type=MESH)
    pl.semaphore_wait(barrier, 2)

    def part(q, sub):
        h = pl.ds(pl.multiple_of(sub * PIECE, PIECE), PIECE)
        return pltpu.make_async_remote_copy(
            src_ref=last_v.at[q, h], dst_ref=recv_v.at[q, h], send_sem=s_sem.at[q, sub], recv_sem=r_sem.at[q, sub],
            device_id={"tp": to[q]}, device_id_type=MESH,
        )

    def mine(sub):
        return sub >= core * early

    for sub in range(C):
        @pl.when(mine(sub))
        def _():
            for q in range(2):
                part(q, sub).start()

    def piece(sub, add):
        for q in range(2):
            def put(i, _):
                h = pl.ds(pl.multiple_of(sub * PIECE + i * 16, 16), 16)
                r = pl.ds(pl.multiple_of(q * H + sub * PIECE + i * 16, 16), 16)
                v = acc_v[r]
                if add:
                    v = v + recv_v[q, h].astype(F32)
                dx_ref[r] = v.astype(BF16)
                return 0

            if add:
                part(q, sub).wait_recv()
            lax.fori_loop(0, PIECE // 16, put, 0)
            if add:
                part(q, sub).wait_send()

    def each(sub, _):
        pl.when(mine(sub))(lambda: piece(sub, True))
        pl.when(jnp.logical_not(mine(sub)))(lambda: piece(sub, False))
        return 0

    lax.fori_loop(0, C, each, 0)


def write_out(k, *refs):
    for mark in refs[2 * k : -1]:
        mark[...] = jnp.zeros_like(mark)
    copies = [pltpu.make_async_copy(refs[i], refs[k + i], refs[-1].at[i]) for i in range(k)]
    for c in copies:
        c.start()
    for c in copies:
        c.wait()


def solution(mesh):
    n = mesh.shape["tp"]

    def body(x, dy, gate, up, w_gate, w_up, w_down):
        R, D = x.shape
        T, F = gate.shape
        H = R // 2
        W = 256
        early = C
        out = lambda *s: jax.ShapeDtypeStruct(s, BF16)
        vmem_spec = pl.BlockSpec(memory_space=pltpu.VMEM)
        any_spec = pl.BlockSpec(memory_space=pl.ANY)
        dma = pltpu.SemaphoreType.DMA
        vmem = lambda s, t: pltpu.VMEM(s, t)
        keep = lambda a: pltpu.with_memory_space_constraint(a, pltpu.VMEM)

        def write(arrays, marks, name):
            k = len(arrays)
            return pl.pallas_call(
                functools.partial(write_out, k),
                out_shape=[out(*a.shape) for a in arrays] + [vmem((8, 128), F32)] * marks,
                in_specs=[vmem_spec] * k,
                out_specs=[any_spec] * k + [vmem_spec] * marks,
                scratch_shapes=[dma((k,))],
                compiler_params=pltpu.CompilerParams(vmem_limit_bytes=2**18),
                name=name,
            )(*(keep(a) for a in arrays))

        *dw, acc, last, _, _, _ = pl.pallas_call(
            functools.partial(kernel, n, early),
            out_shape=[vmem(s, BF16) for s in ((D, F), (D, F), (F, D))]
            + [vmem((R, D), F32), vmem((2, H, D), BF16), out(T, D), out(T, D), out(4, R, D)],
            in_specs=[any_spec] * 7,
            out_specs=[vmem_spec] * 5 + [any_spec] * 3,
            scratch_shapes=[
                pltpu.VMEM((D, 2 * F), BF16),
                pltpu.VMEM((T, 2 * F), BF16),
                pltpu.VMEM((T, F), BF16),
                pltpu.VMEM((2, R, D), BF16),
                pltpu.VMEM((2, 2, R, F), BF16),
                pltpu.VMEM((R, F), F32),
                pltpu.VMEM((2, R, D), BF16),
                pltpu.VMEM((4, H, D), BF16),
                pltpu.VMEM((6, H, D), BF16),
                pltpu.VMEM((2, T, W), BF16),
                dma((2, 13)), dma((2, 13)),
                dma((4,)), dma((4,)),
                dma((4 + 2 * C,)), dma((4 + 2 * C,)),
                dma((3,)), dma((2, 2)), dma((2,)), dma((2,)),
                dma((2,)),
            ],
            compiler_params=pltpu.CompilerParams(collective_id=0, has_side_effects=True, vmem_limit_bytes=199 * 2**18),
            name="mlp_backward",
        )(x, dy, gate, up, w_gate, w_up, w_down)
        *dw, written = write(dw, 1, "write_weight_gradients")
        dx = pl.pallas_call(
            functools.partial(last_hop, n, early),
            out_shape=vmem((R, D), BF16),
            in_specs=[vmem_spec] * 3,
            out_specs=vmem_spec,
            scratch_shapes=[pltpu.VMEM((2, H, D), BF16), dma((2, C)), dma((2, C))],
            compiler_params=pltpu.CompilerParams(collective_id=1, has_side_effects=True, vmem_limit_bytes=2**22),
            name="last_hop",
        )(keep(acc), keep(last), keep(written))
        return (write([dx], 0, "write_dx")[0], *dw)

    tok, col, row = P(("dp", "tp"), None), P("dp", "tp"), P("tp", None)
    wcol = P(None, "tp")
    return jax.shard_map(
        body, mesh=mesh, in_specs=(tok, tok, col, col, wcol, wcol, row), out_specs=(tok, col, col, tok), check_vma=False
    )
```

```python
import functools

import jax
import jax.numpy as jnp
from jax import lax
from jax.experimental import pallas as pl
from jax.experimental.pallas import tpu as pltpu
from jax.sharding import PartitionSpec as P

MESH = pl.DeviceIdType.MESH
BF16, F32 = jnp.bfloat16, jnp.float32
NT = (((1,), (1,)), ((), ()))
TN = (((0,), (0,)), ((), ()))
C = 4


def act(gate, up):
    return jax.nn.gelu(gate) * up


def kernel(
    n, x_ref, dy_ref, gate_ref, up_ref, wg_ref, wu_ref, wd_ref,
    dwg_ref, dwu_ref, dwd_ref, acc_v, last_v, dyg, xg, pbuf,
    wgu_v, dgu_v, hid_v, tile_v, gu_v, dh_v, psend, rsend, rrecv, strip_v,
    ag_s, ag_r, p_s, p_r, q_s, q_r, w_sem, g_sem, t_sem, own_sem, st_sem,
):
    me = lax.axis_index("tp")
    core = lax.rem(me, 2)
    other = 1 - 2 * core
    right, left, far = lax.rem(me + 2, n), lax.rem(me + n - 2, n), lax.rem(me + 4, n)
    partner = me + other
    R, D = dy_ref.shape
    H = R // 2
    F = gate_ref.shape[1]
    T = n * R

    def rows(block, half=None):
        if half is None:
            return pl.ds(pl.multiple_of(block * R, R), R)
        return pl.ds(pl.multiple_of(block * R + half * H, H), H)

    def local(src, dst, sem):
        return pltpu.make_async_copy(src, dst, sem)

    def remote(src, dst, s, r, to):
        return pltpu.make_async_remote_copy(src_ref=src, dst_ref=dst, send_sem=s, recv_sem=r, device_id={"tp": to}, device_id_type=MESH)

    pieces = ((left, 0), (left, 1), (right, 1), (right, 0), (far, 0), (far, 1))
    own_sends = ((right, 0), (right, 1), (left, 1), (left, 0))
    own = (dy_ref, x_ref)
    full = (dyg, xg)

    def ring_own(a, k):
        to, half = own_sends[k]
        return remote(own[a].at[pl.ds(half * H, H)], full[a].at[rows(me, half)], ag_s.at[a, k], ag_r.at[a, k], to)

    def ring_fwd(a, k):
        block, half, to = ((left, 0, right), (right, 1, left))[k - 4]
        ref = full[a].at[rows(block, half)]
        return remote(ref, ref, ag_s.at[a, k], ag_r.at[a, k], to)

    def ring_arrived(a, k):
        block, half = pieces[k]
        ref = full[a].at[rows(block, half)]
        remote(ref, ref, ag_s.at[a, k], ag_r.at[a, k], partner).wait_recv()

    def pair_own(a):
        return remote(own[a], full[a].at[rows(me)], ag_s.at[a, 6], ag_r.at[a, 6], partner)

    def pair_fwd(a, k):
        block, half = pieces[k]
        ref = full[a].at[rows(block, half)]
        return remote(ref, ref, ag_s.at[a, 7 + k], ag_r.at[a, 7 + k], partner)

    def pair_arrived(a, k):
        if k < 0:
            ref = full[a].at[rows(partner)]
            remote(ref, ref, ag_s.at[a, 6], ag_r.at[a, 6], partner).wait_recv()
        else:
            block, half = pieces[k]
            ref = full[a].at[rows(block + other, half)]
            remote(ref, ref, ag_s.at[a, 7 + k], ag_r.at[a, 7 + k], partner).wait_recv()

    wd_v = dwd_ref
    w_copies = (
        local(wd_ref, wd_v, w_sem.at[0]),
        local(wg_ref, wgu_v.at[:, pl.ds(0, F)], w_sem.at[1]),
        local(wu_ref, wgu_v.at[:, pl.ds(F, F)], w_sem.at[2]),
    )

    barrier = pltpu.get_barrier_semaphore()
    for to in (left, right, partner):
        pl.semaphore_signal(barrier, inc=1, device_id={"tp": to}, device_id_type=MESH)
    pl.semaphore_wait(barrier, 3)

    for k in (0, 2, 1, 3):
        ring_own(0, k).start()
    pair_own(0).start()
    pair_own(1).start()

    def block_of(s):
        j = s // 2
        hop = j + j // 2 - 2 * (j // 3)
        return lax.rem(me + 2 * hop, n) + lax.rem(s, 2) * other

    def gate_load(s, slot):
        r = rows(block_of(s))
        return (
            local(gate_ref.at[r], gu_v.at[slot, 0], g_sem.at[slot, 0]),
            local(up_ref.at[r], gu_v.at[slot, 1], g_sem.at[slot, 1]),
        )

    def tile_load(s, slot):
        return local(dyg.at[rows(block_of(s))], tile_v.at[slot], t_sem.at[slot])

    w_copies[0].start()
    local(dy_ref, tile_v.at[0], t_sem.at[0]).start()
    for c in gate_load(0, 0):
        c.start()
    stage = [local(dy_ref, psend.at[0], own_sem.at[0]), local(x_ref, psend.at[1], own_sem.at[1])]
    for c in stage:
        c.start()
    w_copies[1].start()
    w_copies[2].start()
    for c in stage:
        c.wait()
    stage = [local(psend.at[0], dyg.at[rows(me)], own_sem.at[0]), local(psend.at[1], xg.at[rows(me)], own_sem.at[1])]
    for c in stage:
        c.start()
    w_copies[0].wait()

    def step(s, _):
        slot, nxt = lax.rem(s, 2), lax.rem(s + 1, 2)
        r = rows(block_of(s))
        tile_load(s, slot).wait()
        for c in gate_load(s, slot):
            c.wait()
        dh_v[...] = lax.dot_general(tile_v[slot], wd_v[...], NT, preferred_element_type=F32)

        @pl.when(s == 0)
        def _():
            pair_arrived(0, -1)

        @pl.when(s == 1)
        def _():
            for k in (0, 2):
                ring_arrived(0, k)
            for k in (4, 5):
                ring_fwd(0, k).start()
            for k in (0, 2, 1, 3):
                ring_own(1, k).start()
            for k in (0, 2):
                pair_fwd(0, k).start()
            for k in (1, 3):
                ring_arrived(0, k)
                pair_fwd(0, k).start()

        @pl.when(s == 2)
        def _():
            for k in (2, 3):
                pair_arrived(0, k)

        @pl.when(s == 4)
        def _():
            for k in (0, 1):
                pair_arrived(0, k)

        @pl.when(s == 5)
        def _():
            for k in (4, 5):
                ring_arrived(0, k)
                pair_fwd(0, k).start()

        @pl.when(s == 6)
        def _():
            for k in (4, 5):
                pair_arrived(0, k)

        @pl.when(s < n - 1)
        def _():
            tile_load(s + 1, nxt).start()
            for c in gate_load(s + 1, nxt):
                c.start()

        def chunk(i, _):
            m = 16
            q = pl.ds(pl.multiple_of(i * m, m), m)
            o = pl.ds(pl.multiple_of(block_of(s) * R + i * m, m), m)
            hidden, back = jax.vjp(act, gu_v[slot, 0, q].astype(F32), gu_v[slot, 1, q].astype(F32))
            dg, du = back(dh_v[q])
            dgu_v[o, pl.ds(0, F)] = dg.astype(BF16)
            dgu_v[o, pl.ds(F, F)] = du.astype(BF16)
            hid_v[o] = hidden.astype(BF16)
            return 0

        lax.fori_loop(0, R // 16, chunk, 0)
        return 0

    lax.fori_loop(0, n, step, 0)
    for c in stage:
        c.wait()
    for c in w_copies[1:]:
        c.wait()

    NB = 512

    def dx_terms(row0, m, emit):
        def ntile(t, _):
            cols = pl.ds(pl.multiple_of(t * NB, NB), NB)
            emit(cols, lax.dot_general(dgu_v[pl.ds(row0, m)], wgu_v[cols], NT, preferred_element_type=F32))
            return 0

        lax.fori_loop(0, D // NB, ntile, 0)

    targets = (far, right, left, me)

    def p_copy(i):
        return remote(psend.at[i % 2], pbuf.at[i], p_s.at[i], p_r.at[i], partner)

    for i, block in enumerate(targets):
        if i >= 2:
            p_copy(i - 2).wait_send()

        def emit(cols, v, i=i):
            psend[i % 2, :, cols] = v.astype(BF16)

        dx_terms(pl.multiple_of((block + other) * R, R), R, emit)
        p_copy(i).start()

    for k in (0, 2):
        ring_arrived(1, k)
    for k in (4, 5):
        ring_fwd(1, k).start()
    for k in (0, 2):
        pair_fwd(1, k).start()

    def p_load(i, half=None):
        if half is None:
            return local(pbuf.at[i], tile_v.at[i % 2], t_sem.at[i % 2])
        h = pl.ds(half * H, H)
        return local(pbuf.at[i, h], tile_v.at[i % 2, h], t_sem.at[i % 2])

    def p_fetch(i):
        p_copy(i).wait_recv()
        p_load(i).start()

    PIECE = H // C

    def q_src(q):
        return rsend.at[q] if q < 4 else last_v.at[q - 4]

    def q_part(q, sub=None):
        h, k = (pl.ds(0, H), q) if sub is None else (pl.ds(pl.multiple_of(sub * PIECE, PIECE), PIECE), q + 2 * sub)
        return remote(q_src(q).at[h], rrecv.at[q, h], q_s.at[k], q_r.at[k], (right, left)[q % 2])

    def q_parts(q):
        return [q_part(q)] if q < 4 else [q_part(q, sub) for sub in range(C)]

    def ring_sum(q, i, half, add=None):
        h = pl.ds(half * H, H)
        dst = q_src(q)

        def emit(cols, v):
            v = v + tile_v[i % 2, h, cols].astype(F32)
            if add is not None:
                v = v + rrecv[add, :, cols].astype(F32)
            dst[:, cols] = v.astype(BF16)

        dx_terms(pl.multiple_of(targets[i] * R + half * H, H), H, emit)
        if q < 4:
            q_part(q).start()

    p_fetch(0)
    p_fetch(1)
    p_load(0).wait()
    ring_sum(0, 0, 0)
    ring_sum(1, 0, 1)
    p_fetch(2)
    p_load(1).wait()
    ring_sum(2, 1, 1)
    p_fetch(3)
    p_load(2).wait()
    ring_sum(3, 2, 0)
    p_load(3).wait()

    def emit_own(cols, v):
        acc_v[:, cols] = v + tile_v[1, :, cols].astype(F32)

    dx_terms(pl.multiple_of(me * R, R), R, emit_own)

    for k in (1, 3):
        ring_arrived(1, k)
        pair_fwd(1, k).start()

    W = strip_v.shape[2]

    def strip_load(a, t, slot):
        return local(full[a].at[:, pl.ds(pl.multiple_of(t * W, W), W)], strip_v.at[slot], st_sem.at[slot])

    def strips(a, lo, hi, work):
        strip_load(a, lo, lo % 2).start()

        def one(t, _):
            slot = lax.rem(t, 2)
            strip_load(a, t, slot).wait()

            @pl.when(t + 1 < hi)
            def _():
                strip_load(a, t + 1, 1 - slot).start()

            work(slot, pl.ds(pl.multiple_of(t * W, W), W))
            return 0

        lax.fori_loop(lo, hi, one, 0)

    def down_work(slot, part):
        v = lax.dot_general(strip_v[slot], hid_v[...], TN, preferred_element_type=F32)
        dwd_ref[:, part] = v.T.astype(BF16)

    def in_work(slot, part):
        v = lax.dot_general(strip_v[slot], dgu_v[...], TN, preferred_element_type=F32)
        dwg_ref[part] = v[:, :F].astype(BF16)
        dwu_ref[part] = v[:, F:].astype(BF16)

    S = D // W
    strips(0, 0, S, down_work)

    for k in (4, 5):
        ring_arrived(1, k)
        pair_fwd(1, k).start()
    for k in (-1, 0, 1, 2, 3, 4, 5):
        pair_arrived(1, k)

    strips(1, 0, S // 2, in_work)

    for i, half in ((1, 0), (2, 1)):
        p_load(i, half).start()
    for c in q_parts(0) + q_parts(1):
        c.wait_recv()
    for i, half in ((1, 0), (2, 1)):
        p_load(i, half).wait()
    for i in (2, 3):
        p_copy(i).wait_send()
    ring_sum(4, 1, 0, add=0)
    ring_sum(5, 2, 1, add=1)

    @pl.when(core == 1)
    def _():
        for sub in range(C):
            for q in (4, 5):
                q_part(q, sub).start()


    strips(1, S // 2, S, in_work)

    for a in range(2):
        for k in range(4):
            ring_own(a, k).wait_send()
        pair_own(a).wait_send()
        for k in (4, 5):
            ring_fwd(a, k).wait_send()
        for k in range(6):
            pair_fwd(a, k).wait_send()
    for q in range(4):
        q_part(q).wait_send()
    for q in (2, 3):
        q_part(q).wait_recv()

    def settle(i, _):
        h = pl.ds(pl.multiple_of(i * 16, 16), 16)
        for q, base in ((3, 0), (2, H)):
            r = pl.ds(pl.multiple_of(base + i * 16, 16), 16)
            acc_v[r] = acc_v[r] + rrecv[q, h].astype(F32)
        return 0

    lax.fori_loop(0, H // 16, settle, 0)

    @pl.when(core == 1)
    def _():
        def finish(sub, _):
            for q, base in ((4, 0), (5, H)):
                q_part(q, sub).wait_recv()

                def put(i, _):
                    h = pl.ds(pl.multiple_of(sub * PIECE + i * 16, 16), 16)
                    r = pl.ds(pl.multiple_of(base + sub * PIECE + i * 16, 16), 16)
                    acc_v[r] = acc_v[r] + rrecv[q, h].astype(F32)
                    return 0

                lax.fori_loop(0, PIECE // 16, put, 0)
            for q in (4, 5):
                q_part(q, sub).wait_send()
            return 0

        lax.fori_loop(0, C, finish, 0)


def last_hop(n, acc_v, last_v, after_ref, dx_ref, recv_v, s_sem, r_sem):
    me = lax.axis_index("tp")
    core = lax.rem(me, 2)
    to = (lax.rem(me + 2, n), lax.rem(me + n - 2, n))
    H = acc_v.shape[0] // 2
    PIECE = H // C

    barrier = pltpu.get_barrier_semaphore()
    for t in to:
        pl.semaphore_signal(barrier, inc=1, device_id={"tp": t}, device_id_type=MESH)
    pl.semaphore_wait(barrier, 2)

    def part(q, sub):
        h = pl.ds(pl.multiple_of(sub * PIECE, PIECE), PIECE)
        return pltpu.make_async_remote_copy(
            src_ref=last_v.at[q, h], dst_ref=recv_v.at[q, h], send_sem=s_sem.at[q, sub], recv_sem=r_sem.at[q, sub],
            device_id={"tp": to[q]}, device_id_type=MESH,
        )

    def finish(lo, count, add):
        for q in range(2):
            def put(i, _):
                h = pl.ds(pl.multiple_of(lo + i * 16, 16), 16)
                r = pl.ds(pl.multiple_of(q * H + lo + i * 16, 16), 16)
                v = acc_v[r]
                if add:
                    v = v + recv_v[q, h].astype(F32)
                dx_ref[r] = v.astype(BF16)
                return 0

            lax.fori_loop(0, count // 16, put, 0)

    @pl.when(core == 0)
    def _():
        for sub in range(C):
            for q in range(2):
                part(q, sub).start()

        def each(sub, _):
            for q in range(2):
                part(q, sub).wait_recv()
            finish(sub * PIECE, PIECE, True)
            for q in range(2):
                part(q, sub).wait_send()
            return 0

        lax.fori_loop(0, C, each, 0)

    @pl.when(core == 1)
    def _():
        finish(0, H, False)


def write_out(*refs):
    k = (len(refs) - 2) // 2
    refs[-2][...] = jnp.zeros_like(refs[-2])
    copies = [pltpu.make_async_copy(refs[i], refs[k + i], refs[-1].at[i]) for i in range(k)]
    for c in copies:
        c.start()
    for c in copies:
        c.wait()


def solution(mesh):
    n = mesh.shape["tp"]

    def body(x, dy, gate, up, w_gate, w_up, w_down):
        R, D = x.shape
        T, F = gate.shape
        H = R // 2
        W = 256
        out = lambda *s: jax.ShapeDtypeStruct(s, BF16)
        vmem_spec = pl.BlockSpec(memory_space=pltpu.VMEM)
        any_spec = pl.BlockSpec(memory_space=pl.ANY)
        dma = pltpu.SemaphoreType.DMA
        vmem = lambda s, t: pltpu.VMEM(s, t)
        keep = lambda a: pltpu.with_memory_space_constraint(a, pltpu.VMEM)

        *dw, acc, last, _, _, _ = pl.pallas_call(
            functools.partial(kernel, n),
            out_shape=[vmem(s, BF16) for s in ((D, F), (D, F), (F, D))]
            + [vmem((R, D), F32), vmem((2, H, D), BF16), out(T, D), out(T, D), out(4, R, D)],
            in_specs=[any_spec] * 7,
            out_specs=[vmem_spec] * 5 + [any_spec] * 3,
            scratch_shapes=[
                pltpu.VMEM((D, 2 * F), BF16),
                pltpu.VMEM((T, 2 * F), BF16),
                pltpu.VMEM((T, F), BF16),
                pltpu.VMEM((2, R, D), BF16),
                pltpu.VMEM((2, 2, R, F), BF16),
                pltpu.VMEM((R, F), F32),
                pltpu.VMEM((2, R, D), BF16),
                pltpu.VMEM((4, H, D), BF16),
                pltpu.VMEM((6, H, D), BF16),
                pltpu.VMEM((2, T, W), BF16),
                dma((2, 13)), dma((2, 13)),
                dma((4,)), dma((4,)),
                dma((4 + 2 * C,)), dma((4 + 2 * C,)),
                dma((3,)), dma((2, 2)), dma((2,)), dma((2,)),
                dma((2,)),
            ],
            compiler_params=pltpu.CompilerParams(collective_id=0, has_side_effects=True, vmem_limit_bytes=199 * 2**18),
            name="mlp_backward",
        )(x, dy, gate, up, w_gate, w_up, w_down)
        *dw, written = pl.pallas_call(
            write_out,
            out_shape=[out(*a.shape) for a in dw] + [vmem((8, 128), F32)],
            in_specs=[vmem_spec] * len(dw),
            out_specs=[any_spec] * len(dw) + [vmem_spec],
            scratch_shapes=[dma((len(dw),))],
            compiler_params=pltpu.CompilerParams(vmem_limit_bytes=2**18),
            name="write_weight_gradients",
        )(*(keep(a) for a in dw))
        dx = pl.pallas_call(
            functools.partial(last_hop, n),
            out_shape=vmem((R, D), BF16),
            in_specs=[vmem_spec] * 3,
            out_specs=vmem_spec,
            scratch_shapes=[pltpu.VMEM((2, H, D), BF16), dma((2, C)), dma((2, C))],
            compiler_params=pltpu.CompilerParams(collective_id=1, has_side_effects=True, vmem_limit_bytes=2**22),
            name="last_hop",
        )(keep(acc), keep(last), keep(written))
        return (dx, *dw)

    tok, col, row = P(("dp", "tp"), None), P("dp", "tp"), P("tp", None)
    wcol = P(None, "tp")
    return jax.shard_map(
        body, mesh=mesh, in_specs=(tok, tok, col, col, wcol, wcol, row), out_specs=(tok, col, col, tok), check_vma=False
    )
```

```python
import functools

import jax
import jax.numpy as jnp
from jax import lax
from jax.experimental import pallas as pl
from jax.experimental.pallas import tpu as pltpu
from jax.sharding import PartitionSpec as P

MESH = pl.DeviceIdType.MESH
BF16, F32 = jnp.bfloat16, jnp.float32
NT = (((1,), (1,)), ((), ()))
TN = (((0,), (0,)), ((), ()))
C = 4


def act(gate, up):
    return jax.nn.gelu(gate) * up


def kernel(
    n, x_ref, dy_ref, gate_ref, up_ref, wg_ref, wu_ref, wd_ref,
    dwg_ref, dwu_ref, dwd_ref, acc_v, last_v, dyg, xg, pbuf,
    wgu_v, dgu_v, hid_v, tile_v, gu_v, dh_v, psend, rsend, rrecv, strip_v,
    ag_s, ag_r, p_s, p_r, q_s, q_r, w_sem, g_sem, t_sem, own_sem, st_sem,
):
    me = lax.axis_index("tp")
    core = lax.rem(me, 2)
    other = 1 - 2 * core
    right, left, far = lax.rem(me + 2, n), lax.rem(me + n - 2, n), lax.rem(me + 4, n)
    partner = me + other
    R, D = dy_ref.shape
    H = R // 2
    F = gate_ref.shape[1]
    T = n * R

    def rows(block, half=None):
        if half is None:
            return pl.ds(pl.multiple_of(block * R, R), R)
        return pl.ds(pl.multiple_of(block * R + half * H, H), H)

    def local(src, dst, sem):
        return pltpu.make_async_copy(src, dst, sem)

    def remote(src, dst, s, r, to):
        return pltpu.make_async_remote_copy(src_ref=src, dst_ref=dst, send_sem=s, recv_sem=r, device_id={"tp": to}, device_id_type=MESH)

    pieces = ((left, 0), (left, 1), (right, 1), (right, 0), (far, 0), (far, 1))
    own_sends = ((right, 0), (right, 1), (left, 1), (left, 0))
    own = (dy_ref, x_ref)
    full = (dyg, xg)

    def ring_own(a, k):
        to, half = own_sends[k]
        return remote(own[a].at[pl.ds(half * H, H)], full[a].at[rows(me, half)], ag_s.at[a, k], ag_r.at[a, k], to)

    def ring_fwd(a, k):
        block, half, to = ((left, 0, right), (right, 1, left))[k - 4]
        ref = full[a].at[rows(block, half)]
        return remote(ref, ref, ag_s.at[a, k], ag_r.at[a, k], to)

    def ring_arrived(a, k):
        block, half = pieces[k]
        ref = full[a].at[rows(block, half)]
        remote(ref, ref, ag_s.at[a, k], ag_r.at[a, k], partner).wait_recv()

    def pair_own(a):
        return remote(own[a], full[a].at[rows(me)], ag_s.at[a, 6], ag_r.at[a, 6], partner)

    def pair_fwd(a, k):
        block, half = pieces[k]
        ref = full[a].at[rows(block, half)]
        return remote(ref, ref, ag_s.at[a, 7 + k], ag_r.at[a, 7 + k], partner)

    def pair_arrived(a, k):
        if k < 0:
            ref = full[a].at[rows(partner)]
            remote(ref, ref, ag_s.at[a, 6], ag_r.at[a, 6], partner).wait_recv()
        else:
            block, half = pieces[k]
            ref = full[a].at[rows(block + other, half)]
            remote(ref, ref, ag_s.at[a, 7 + k], ag_r.at[a, 7 + k], partner).wait_recv()

    wd_v = dwd_ref
    w_copies = (
        local(wd_ref, wd_v, w_sem.at[0]),
        local(wg_ref, wgu_v.at[:, pl.ds(0, F)], w_sem.at[1]),
        local(wu_ref, wgu_v.at[:, pl.ds(F, F)], w_sem.at[2]),
    )

    barrier = pltpu.get_barrier_semaphore()
    for to in (left, right, partner):
        pl.semaphore_signal(barrier, inc=1, device_id={"tp": to}, device_id_type=MESH)
    pl.semaphore_wait(barrier, 3)

    for k in (0, 2, 1, 3):
        ring_own(0, k).start()
    pair_own(0).start()
    pair_own(1).start()

    def block_of(s):
        j = s // 2
        hop = j + j // 2 - 2 * (j // 3)
        return lax.rem(me + 2 * hop, n) + lax.rem(s, 2) * other

    def gate_load(s, slot):
        r = rows(block_of(s))
        return (
            local(gate_ref.at[r], gu_v.at[slot, 0], g_sem.at[slot, 0]),
            local(up_ref.at[r], gu_v.at[slot, 1], g_sem.at[slot, 1]),
        )

    def tile_load(s, slot):
        return local(dyg.at[rows(block_of(s))], tile_v.at[slot], t_sem.at[slot])

    w_copies[0].start()
    local(dy_ref, tile_v.at[0], t_sem.at[0]).start()
    for c in gate_load(0, 0):
        c.start()
    stage = [local(dy_ref, psend.at[0], own_sem.at[0]), local(x_ref, psend.at[1], own_sem.at[1])]
    for c in stage:
        c.start()
    w_copies[1].start()
    w_copies[2].start()
    for c in stage:
        c.wait()
    stage = [local(psend.at[0], dyg.at[rows(me)], own_sem.at[0]), local(psend.at[1], xg.at[rows(me)], own_sem.at[1])]
    for c in stage:
        c.start()
    w_copies[0].wait()

    def step(s, _):
        slot, nxt = lax.rem(s, 2), lax.rem(s + 1, 2)
        r = rows(block_of(s))
        tile_load(s, slot).wait()
        for c in gate_load(s, slot):
            c.wait()
        dh_v[...] = lax.dot_general(tile_v[slot], wd_v[...], NT, preferred_element_type=F32)

        @pl.when(s == 0)
        def _():
            pair_arrived(0, -1)

        @pl.when(s == 1)
        def _():
            for k in (0, 2):
                ring_arrived(0, k)
            for k in (4, 5):
                ring_fwd(0, k).start()
            for k in (0, 2, 1, 3):
                ring_own(1, k).start()
            for k in (0, 2):
                pair_fwd(0, k).start()
            for k in (1, 3):
                ring_arrived(0, k)
                pair_fwd(0, k).start()

        @pl.when(s == 2)
        def _():
            for k in (2, 3):
                pair_arrived(0, k)

        @pl.when(s == 4)
        def _():
            for k in (0, 1):
                pair_arrived(0, k)

        @pl.when(s == 5)
        def _():
            for k in (4, 5):
                ring_arrived(0, k)
                pair_fwd(0, k).start()

        @pl.when(s == 6)
        def _():
            for k in (4, 5):
                pair_arrived(0, k)

        @pl.when(s < n - 1)
        def _():
            tile_load(s + 1, nxt).start()
            for c in gate_load(s + 1, nxt):
                c.start()

        def chunk(i, _):
            m = 16
            q = pl.ds(pl.multiple_of(i * m, m), m)
            o = pl.ds(pl.multiple_of(block_of(s) * R + i * m, m), m)
            hidden, back = jax.vjp(act, gu_v[slot, 0, q].astype(F32), gu_v[slot, 1, q].astype(F32))
            dg, du = back(dh_v[q])
            dgu_v[o, pl.ds(0, F)] = dg.astype(BF16)
            dgu_v[o, pl.ds(F, F)] = du.astype(BF16)
            hid_v[o] = hidden.astype(BF16)
            return 0

        lax.fori_loop(0, R // 16, chunk, 0)
        return 0

    lax.fori_loop(0, n, step, 0)
    for c in stage:
        c.wait()
    for c in w_copies[1:]:
        c.wait()

    NB = 512

    def dx_terms(row0, m, emit):
        def ntile(t, _):
            cols = pl.ds(pl.multiple_of(t * NB, NB), NB)
            emit(cols, lax.dot_general(dgu_v[pl.ds(row0, m)], wgu_v[cols], NT, preferred_element_type=F32))
            return 0

        lax.fori_loop(0, D // NB, ntile, 0)

    targets = (far, right, left, me)

    def p_copy(i):
        return remote(psend.at[i % 2], pbuf.at[i], p_s.at[i], p_r.at[i], partner)

    for i, block in enumerate(targets):
        if i >= 2:
            p_copy(i - 2).wait_send()

        def emit(cols, v, i=i):
            psend[i % 2, :, cols] = v.astype(BF16)

        dx_terms(pl.multiple_of((block + other) * R, R), R, emit)
        if i >= 1:
            p_copy(i - 1).start()

    for k in (0, 2):
        ring_arrived(1, k)
    for k in (4, 5):
        ring_fwd(1, k).start()
    for k in (0, 2):
        pair_fwd(1, k).start()
    p_copy(3).start()

    def p_load(i, half=None):
        if half is None:
            return local(pbuf.at[i], tile_v.at[i % 2], t_sem.at[i % 2])
        h = pl.ds(half * H, H)
        return local(pbuf.at[i, h], tile_v.at[i % 2, h], t_sem.at[i % 2])

    def p_fetch(i):
        p_copy(i).wait_recv()
        p_load(i).start()

    PIECE = H // C

    def q_src(q):
        return rsend.at[q] if q < 4 else last_v.at[q - 4]

    def q_part(q, sub=None):
        h, k = (pl.ds(0, H), q) if sub is None else (pl.ds(pl.multiple_of(sub * PIECE, PIECE), PIECE), q + 2 * sub)
        return remote(q_src(q).at[h], rrecv.at[q, h], q_s.at[k], q_r.at[k], (right, left)[q % 2])

    def q_parts(q):
        return [q_part(q)] if q < 4 else [q_part(q, sub) for sub in range(C)]

    def ring_sum(q, i, half, add=None):
        h = pl.ds(half * H, H)
        dst = q_src(q)

        def emit(cols, v):
            v = v + tile_v[i % 2, h, cols].astype(F32)
            if add is not None:
                v = v + rrecv[add, :, cols].astype(F32)
            dst[:, cols] = v.astype(BF16)

        dx_terms(pl.multiple_of(targets[i] * R + half * H, H), H, emit)
        if 1 <= q < 4:
            q_part(q - 1).start()

    p_fetch(0)
    p_fetch(1)
    p_load(0).wait()
    ring_sum(0, 0, 0)
    ring_sum(1, 0, 1)
    p_fetch(2)
    p_load(1).wait()
    ring_sum(2, 1, 1)
    p_fetch(3)
    p_load(2).wait()
    ring_sum(3, 2, 0)
    p_load(3).wait()

    def emit_own(cols, v):
        acc_v[:, cols] = v + tile_v[1, :, cols].astype(F32)

    dx_terms(pl.multiple_of(me * R, R), R, emit_own)
    q_part(3).start()

    for k in (1, 3):
        ring_arrived(1, k)
        pair_fwd(1, k).start()

    W = strip_v.shape[2]

    def strip_load(a, t, slot):
        return local(full[a].at[:, pl.ds(pl.multiple_of(t * W, W), W)], strip_v.at[slot], st_sem.at[slot])

    def strips(a, lo, hi, work, after_first=lambda: None):
        strip_load(a, lo, lo % 2).start()

        def one(t, _):
            slot = lax.rem(t, 2)
            strip_load(a, t, slot).wait()

            @pl.when(t + 1 < hi)
            def _():
                strip_load(a, t + 1, 1 - slot).start()

            work(slot, pl.ds(pl.multiple_of(t * W, W), W))
            pl.when(t == lo)(after_first)
            return 0

        lax.fori_loop(lo, hi, one, 0)

    def down_work(slot, part):
        v = lax.dot_general(strip_v[slot], hid_v[...], TN, preferred_element_type=F32)
        dwd_ref[:, part] = v.T.astype(BF16)

    def in_work(slot, part):
        v = lax.dot_general(strip_v[slot], dgu_v[...], TN, preferred_element_type=F32)
        dwg_ref[part] = v[:, :F].astype(BF16)
        dwu_ref[part] = v[:, F:].astype(BF16)

    S = D // W
    strips(0, 0, S, down_work)

    for k in (4, 5):
        ring_arrived(1, k)
        pair_fwd(1, k).start()
    for k in (-1, 0, 1, 2, 3, 4, 5):
        pair_arrived(1, k)

    strips(1, 0, S // 2, in_work)

    for i, half in ((1, 0), (2, 1)):
        p_load(i, half).start()
    for c in q_parts(0) + q_parts(1):
        c.wait_recv()
    for i, half in ((1, 0), (2, 1)):
        p_load(i, half).wait()
    for i in (2, 3):
        p_copy(i).wait_send()
    ring_sum(4, 1, 0, add=0)
    ring_sum(5, 2, 1, add=1)

    def send_last():
        @pl.when(core == 1)
        def _():
            for sub in range(C):
                for q in (4, 5):
                    q_part(q, sub).start()

    strips(1, S // 2, S, in_work, send_last)

    for a in range(2):
        for k in range(4):
            ring_own(a, k).wait_send()
        pair_own(a).wait_send()
        for k in (4, 5):
            ring_fwd(a, k).wait_send()
        for k in range(6):
            pair_fwd(a, k).wait_send()
    for q in range(4):
        q_part(q).wait_send()
    for q in (2, 3):
        q_part(q).wait_recv()

    def settle(i, _):
        h = pl.ds(pl.multiple_of(i * 16, 16), 16)
        for q, base in ((3, 0), (2, H)):
            r = pl.ds(pl.multiple_of(base + i * 16, 16), 16)
            acc_v[r] = acc_v[r] + rrecv[q, h].astype(F32)
        return 0

    lax.fori_loop(0, H // 16, settle, 0)

    @pl.when(core == 1)
    def _():
        def finish(sub, _):
            for q, base in ((4, 0), (5, H)):
                q_part(q, sub).wait_recv()

                def put(i, _):
                    h = pl.ds(pl.multiple_of(sub * PIECE + i * 16, 16), 16)
                    r = pl.ds(pl.multiple_of(base + sub * PIECE + i * 16, 16), 16)
                    acc_v[r] = acc_v[r] + rrecv[q, h].astype(F32)
                    return 0

                lax.fori_loop(0, PIECE // 16, put, 0)
            for q in (4, 5):
                q_part(q, sub).wait_send()
            return 0

        lax.fori_loop(0, C, finish, 0)


def last_hop(n, acc_v, last_v, after_ref, dx_ref, recv_v, s_sem, r_sem):
    me = lax.axis_index("tp")
    core = lax.rem(me, 2)
    to = (lax.rem(me + 2, n), lax.rem(me + n - 2, n))
    H = acc_v.shape[0] // 2
    PIECE = H // C

    barrier = pltpu.get_barrier_semaphore()
    for t in to:
        pl.semaphore_signal(barrier, inc=1, device_id={"tp": t}, device_id_type=MESH)
    pl.semaphore_wait(barrier, 2)

    def part(q, sub):
        h = pl.ds(pl.multiple_of(sub * PIECE, PIECE), PIECE)
        return pltpu.make_async_remote_copy(
            src_ref=last_v.at[q, h], dst_ref=recv_v.at[q, h], send_sem=s_sem.at[q, sub], recv_sem=r_sem.at[q, sub],
            device_id={"tp": to[q]}, device_id_type=MESH,
        )

    def finish(lo, count, add):
        for q in range(2):
            def put(i, _):
                h = pl.ds(pl.multiple_of(lo + i * 16, 16), 16)
                r = pl.ds(pl.multiple_of(q * H + lo + i * 16, 16), 16)
                v = acc_v[r]
                if add:
                    v = v + recv_v[q, h].astype(F32)
                dx_ref[r] = v.astype(BF16)
                return 0

            lax.fori_loop(0, count // 16, put, 0)

    @pl.when(core == 0)
    def _():
        for sub in range(C):
            for q in range(2):
                part(q, sub).start()

        def each(sub, _):
            for q in range(2):
                part(q, sub).wait_recv()
            finish(sub * PIECE, PIECE, True)
            for q in range(2):
                part(q, sub).wait_send()
            return 0

        lax.fori_loop(0, C, each, 0)

    @pl.when(core == 1)
    def _():
        finish(0, H, False)


def write_out(*refs):
    k = (len(refs) - 2) // 2
    refs[-2][...] = jnp.zeros_like(refs[-2])
    copies = [pltpu.make_async_copy(refs[i], refs[k + i], refs[-1].at[i]) for i in range(k)]
    for c in copies:
        c.start()
    for c in copies:
        c.wait()


def solution(mesh):
    n = mesh.shape["tp"]

    def body(x, dy, gate, up, w_gate, w_up, w_down):
        R, D = x.shape
        T, F = gate.shape
        H = R // 2
        W = 256
        out = lambda *s: jax.ShapeDtypeStruct(s, BF16)
        vmem_spec = pl.BlockSpec(memory_space=pltpu.VMEM)
        any_spec = pl.BlockSpec(memory_space=pl.ANY)
        dma = pltpu.SemaphoreType.DMA
        vmem = lambda s, t: pltpu.VMEM(s, t)
        keep = lambda a: pltpu.with_memory_space_constraint(a, pltpu.VMEM)

        *dw, acc, last, _, _, _ = pl.pallas_call(
            functools.partial(kernel, n),
            out_shape=[vmem(s, BF16) for s in ((D, F), (D, F), (F, D))]
            + [vmem((R, D), F32), vmem((2, H, D), BF16), out(T, D), out(T, D), out(4, R, D)],
            in_specs=[any_spec] * 7,
            out_specs=[vmem_spec] * 5 + [any_spec] * 3,
            scratch_shapes=[
                pltpu.VMEM((D, 2 * F), BF16),
                pltpu.VMEM((T, 2 * F), BF16),
                pltpu.VMEM((T, F), BF16),
                pltpu.VMEM((2, R, D), BF16),
                pltpu.VMEM((2, 2, R, F), BF16),
                pltpu.VMEM((R, F), F32),
                pltpu.VMEM((2, R, D), BF16),
                pltpu.VMEM((4, H, D), BF16),
                pltpu.VMEM((6, H, D), BF16),
                pltpu.VMEM((2, T, W), BF16),
                dma((2, 13)), dma((2, 13)),
                dma((4,)), dma((4,)),
                dma((4 + 2 * C,)), dma((4 + 2 * C,)),
                dma((3,)), dma((2, 2)), dma((2,)), dma((2,)),
                dma((2,)),
            ],
            compiler_params=pltpu.CompilerParams(collective_id=0, has_side_effects=True, vmem_limit_bytes=199 * 2**18),
            name="mlp_backward",
        )(x, dy, gate, up, w_gate, w_up, w_down)
        *dw, written = pl.pallas_call(
            write_out,
            out_shape=[out(*a.shape) for a in dw] + [vmem((8, 128), F32)],
            in_specs=[vmem_spec] * len(dw),
            out_specs=[any_spec] * len(dw) + [vmem_spec],
            scratch_shapes=[dma((len(dw),))],
            compiler_params=pltpu.CompilerParams(vmem_limit_bytes=2**18),
            name="write_weight_gradients",
        )(*(keep(a) for a in dw))
        dx = pl.pallas_call(
            functools.partial(last_hop, n),
            out_shape=vmem((R, D), BF16),
            in_specs=[vmem_spec] * 3,
            out_specs=vmem_spec,
            scratch_shapes=[pltpu.VMEM((2, H, D), BF16), dma((2, C)), dma((2, C))],
            compiler_params=pltpu.CompilerParams(collective_id=1, has_side_effects=True, vmem_limit_bytes=2**22),
            name="last_hop",
        )(keep(acc), keep(last), keep(written))
        return (dx, *dw)

    tok, col, row = P(("dp", "tp"), None), P("dp", "tp"), P("tp", None)
    wcol = P(None, "tp")
    return jax.shard_map(
        body, mesh=mesh, in_specs=(tok, tok, col, col, wcol, wcol, row), out_specs=(tok, col, col, tok), check_vma=False
    )
```

```python
import functools

import jax
import jax.numpy as jnp
from jax import lax
from jax.experimental import pallas as pl
from jax.experimental.pallas import tpu as pltpu
from jax.sharding import PartitionSpec as P

MESH = pl.DeviceIdType.MESH
BF16, F32 = jnp.bfloat16, jnp.float32
NT = (((1,), (1,)), ((), ()))
TN = (((0,), (0,)), ((), ()))
C = 4


def act(gate, up):
    return jax.nn.gelu(gate) * up


def kernel(
    n, x_ref, dy_ref, gate_ref, up_ref, wg_ref, wu_ref, wd_ref,
    dwg_ref, dwu_ref, dwd_ref, acc_v, last_v, dyg, xg, pbuf,
    wgu_v, dgu_v, hid_v, tile_v, gu_v, dh_v, psend, rsend, rrecv, strip_v,
    ag_s, ag_r, p_s, p_r, q_s, q_r, w_sem, g_sem, t_sem, own_sem, st_sem,
):
    me = lax.axis_index("tp")
    core = lax.rem(me, 2)
    other = 1 - 2 * core
    right, left, far = lax.rem(me + 2, n), lax.rem(me + n - 2, n), lax.rem(me + 4, n)
    partner = me + other
    R, D = dy_ref.shape
    H = R // 2
    F = gate_ref.shape[1]
    T = n * R

    def rows(block, half=None):
        if half is None:
            return pl.ds(pl.multiple_of(block * R, R), R)
        return pl.ds(pl.multiple_of(block * R + half * H, H), H)

    def local(src, dst, sem):
        return pltpu.make_async_copy(src, dst, sem)

    def remote(src, dst, s, r, to):
        return pltpu.make_async_remote_copy(src_ref=src, dst_ref=dst, send_sem=s, recv_sem=r, device_id={"tp": to}, device_id_type=MESH)

    pieces = ((left, 0), (left, 1), (right, 1), (right, 0), (far, 0), (far, 1))
    own_sends = ((right, 0), (right, 1), (left, 1), (left, 0))
    own = (dy_ref, x_ref)
    full = (dyg, xg)

    def ring_own(a, k):
        to, half = own_sends[k]
        return remote(own[a].at[pl.ds(half * H, H)], full[a].at[rows(me, half)], ag_s.at[a, k], ag_r.at[a, k], to)

    def ring_fwd(a, k):
        block, half, to = ((left, 0, right), (right, 1, left))[k - 4]
        ref = full[a].at[rows(block, half)]
        return remote(ref, ref, ag_s.at[a, k], ag_r.at[a, k], to)

    def ring_arrived(a, k):
        block, half = pieces[k]
        ref = full[a].at[rows(block, half)]
        remote(ref, ref, ag_s.at[a, k], ag_r.at[a, k], partner).wait_recv()

    def pair_own(a):
        return remote(own[a], full[a].at[rows(me)], ag_s.at[a, 6], ag_r.at[a, 6], partner)

    def pair_fwd(a, k):
        block, half = pieces[k]
        ref = full[a].at[rows(block, half)]
        return remote(ref, ref, ag_s.at[a, 7 + k], ag_r.at[a, 7 + k], partner)

    def pair_arrived(a, k):
        if k < 0:
            ref = full[a].at[rows(partner)]
            remote(ref, ref, ag_s.at[a, 6], ag_r.at[a, 6], partner).wait_recv()
        else:
            block, half = pieces[k]
            ref = full[a].at[rows(block + other, half)]
            remote(ref, ref, ag_s.at[a, 7 + k], ag_r.at[a, 7 + k], partner).wait_recv()

    wd_v = dwd_ref
    w_copies = (
        local(wd_ref, wd_v, w_sem.at[0]),
        local(wg_ref, wgu_v.at[:, pl.ds(0, F)], w_sem.at[1]),
        local(wu_ref, wgu_v.at[:, pl.ds(F, F)], w_sem.at[2]),
    )

    barrier = pltpu.get_barrier_semaphore()
    for to in (left, right, partner):
        pl.semaphore_signal(barrier, inc=1, device_id={"tp": to}, device_id_type=MESH)
    pl.semaphore_wait(barrier, 3)

    for k in (0, 2, 1, 3):
        ring_own(0, k).start()
    pair_own(0).start()
    pair_own(1).start()

    def block_of(s):
        j = s // 2
        hop = j + j // 2 - 2 * (j // 3)
        return lax.rem(me + 2 * hop, n) + lax.rem(s, 2) * other

    def gate_load(s, slot):
        r = rows(block_of(s))
        return (
            local(gate_ref.at[r], gu_v.at[slot, 0], g_sem.at[slot, 0]),
            local(up_ref.at[r], gu_v.at[slot, 1], g_sem.at[slot, 1]),
        )

    def tile_load(s, slot):
        return local(dyg.at[rows(block_of(s))], tile_v.at[slot], t_sem.at[slot])

    w_copies[0].start()
    local(dy_ref, tile_v.at[0], t_sem.at[0]).start()
    for c in gate_load(0, 0):
        c.start()
    stage = [local(dy_ref, psend.at[0], own_sem.at[0]), local(x_ref, psend.at[1], own_sem.at[1])]
    for c in stage:
        c.start()
    w_copies[1].start()
    w_copies[2].start()
    keep_own = [local(psend.at[0], dyg.at[rows(me)], own_sem.at[0]), local(psend.at[1], xg.at[rows(me)], own_sem.at[1])]
    w_copies[0].wait()

    def step(s, _):
        slot, nxt = lax.rem(s, 2), lax.rem(s + 1, 2)
        r = rows(block_of(s))
        tile_load(s, slot).wait()
        for c in gate_load(s, slot):
            c.wait()
        dh_v[...] = lax.dot_general(tile_v[slot], wd_v[...], NT, preferred_element_type=F32)

        @pl.when(s == 0)
        def _():
            for c in stage:
                c.wait()
            for c in keep_own:
                c.start()
            pair_arrived(0, -1)

        @pl.when(s == 1)
        def _():
            for k in (0, 2):
                ring_arrived(0, k)
            for k in (4, 5):
                ring_fwd(0, k).start()
            for k in (0, 2, 1, 3):
                ring_own(1, k).start()
            for k in (0, 2):
                pair_fwd(0, k).start()
            for k in (1, 3):
                ring_arrived(0, k)
                pair_fwd(0, k).start()

        @pl.when(s == 2)
        def _():
            for k in (2, 3):
                pair_arrived(0, k)

        @pl.when(s == 4)
        def _():
            for k in (0, 1):
                pair_arrived(0, k)

        @pl.when(s == 5)
        def _():
            for k in (4, 5):
                ring_arrived(0, k)
                pair_fwd(0, k).start()

        @pl.when(s == 6)
        def _():
            for k in (4, 5):
                pair_arrived(0, k)

        @pl.when(s < n - 1)
        def _():
            tile_load(s + 1, nxt).start()
            for c in gate_load(s + 1, nxt):
                c.start()

        def chunk(i, _):
            m = 16
            q = pl.ds(pl.multiple_of(i * m, m), m)
            o = pl.ds(pl.multiple_of(block_of(s) * R + i * m, m), m)
            hidden, back = jax.vjp(act, gu_v[slot, 0, q].astype(F32), gu_v[slot, 1, q].astype(F32))
            dg, du = back(dh_v[q])
            dgu_v[o, pl.ds(0, F)] = dg.astype(BF16)
            dgu_v[o, pl.ds(F, F)] = du.astype(BF16)
            hid_v[o] = hidden.astype(BF16)
            return 0

        lax.fori_loop(0, R // 16, chunk, 0)
        return 0

    lax.fori_loop(0, n, step, 0)
    for c in keep_own:
        c.wait()
    for c in w_copies[1:]:
        c.wait()

    W = strip_v.shape[2]

    def strip_load(a, t, slot):
        return local(full[a].at[:, pl.ds(pl.multiple_of(t * W, W), W)], strip_v.at[slot], st_sem.at[slot])

    NB = 512

    def dx_terms(row0, m, emit):
        def ntile(t, _):
            cols = pl.ds(pl.multiple_of(t * NB, NB), NB)
            emit(cols, lax.dot_general(dgu_v[pl.ds(row0, m)], wgu_v[cols], NT, preferred_element_type=F32))
            return 0

        lax.fori_loop(0, D // NB, ntile, 0)

    targets = (far, right, left, me)

    def p_copy(i):
        return remote(psend.at[i % 2], pbuf.at[i], p_s.at[i], p_r.at[i], partner)

    for i, block in enumerate(targets):
        if i >= 2:
            p_copy(i - 2).wait_send()

        def emit(cols, v, i=i):
            psend[i % 2, :, cols] = v.astype(BF16)

        dx_terms(pl.multiple_of((block + other) * R, R), R, emit)
        if i >= 1:
            p_copy(i - 1).start()

    for k in (0, 2):
        ring_arrived(1, k)
    for k in (4, 5):
        ring_fwd(1, k).start()
    for k in (0, 2):
        pair_fwd(1, k).start()
    p_copy(3).start()

    def p_load(i, half=None):
        if half is None:
            return local(pbuf.at[i], tile_v.at[i % 2], t_sem.at[i % 2])
        h = pl.ds(half * H, H)
        return local(pbuf.at[i, h], tile_v.at[i % 2, h], t_sem.at[i % 2])

    def p_fetch(i):
        p_copy(i).wait_recv()
        p_load(i).start()

    PIECE = H // C

    def q_src(q):
        return rsend.at[q] if q < 4 else last_v.at[q - 4]

    def q_part(q, sub=None):
        h, k = (pl.ds(0, H), q) if sub is None else (pl.ds(pl.multiple_of(sub * PIECE, PIECE), PIECE), q + 2 * sub)
        return remote(q_src(q).at[h], rrecv.at[q, h], q_s.at[k], q_r.at[k], (right, left)[q % 2])

    def q_parts(q):
        return [q_part(q)] if q < 4 else [q_part(q, sub) for sub in range(C)]

    def ring_sum(q, i, half, add=None):
        h = pl.ds(half * H, H)
        dst = q_src(q)

        def emit(cols, v):
            v = v + tile_v[i % 2, h, cols].astype(F32)
            if add is not None:
                v = v + rrecv[add, :, cols].astype(F32)
            dst[:, cols] = v.astype(BF16)

        dx_terms(pl.multiple_of(targets[i] * R + half * H, H), H, emit)
        if 1 <= q < 4:
            q_part(q - 1).start()

    p_fetch(0)
    p_fetch(1)
    p_load(0).wait()
    ring_sum(0, 0, 0)
    ring_sum(1, 0, 1)
    p_fetch(2)
    p_load(1).wait()
    ring_sum(2, 1, 1)
    p_fetch(3)
    p_load(2).wait()
    ring_sum(3, 2, 0)
    p_load(3).wait()

    def emit_own(cols, v):
        acc_v[:, cols] = v + tile_v[1, :, cols].astype(F32)

    strip_load(0, 0, 0).start()
    dx_terms(pl.multiple_of(me * R, R), R, emit_own)
    q_part(3).start()

    for k in (1, 3):
        ring_arrived(1, k)
        pair_fwd(1, k).start()

    def strips(a, lo, hi, work, after_first=lambda: None):
        def one(t, _):
            slot = lax.rem(t, 2)
            strip_load(a, t, slot).wait()

            @pl.when(t + 1 < hi)
            def _():
                strip_load(a, t + 1, 1 - slot).start()

            work(slot, pl.ds(pl.multiple_of(t * W, W), W))
            pl.when(t == lo)(after_first)
            return 0

        lax.fori_loop(lo, hi, one, 0)

    def down_work(slot, part):
        v = lax.dot_general(strip_v[slot], hid_v[...], TN, preferred_element_type=F32)
        dwd_ref[:, part] = v.T.astype(BF16)

    def in_work(slot, part):
        v = lax.dot_general(strip_v[slot], dgu_v[...], TN, preferred_element_type=F32)
        dwg_ref[part] = v[:, :F].astype(BF16)
        dwu_ref[part] = v[:, F:].astype(BF16)

    S = D // W
    strips(0, 0, S, down_work)

    for k in (4, 5):
        ring_arrived(1, k)
        pair_fwd(1, k).start()
    for k in (-1, 0, 1, 2, 3, 4, 5):
        pair_arrived(1, k)

    strip_load(1, 0, 0).start()
    for i, half in ((1, 0), (2, 1)):
        p_load(i, half).start()
    strips(1, 0, S // 2, in_work)

    strip_load(1, S // 2, S // 2 % 2).start()
    for c in q_parts(0) + q_parts(1):
        c.wait_recv()
    for i, half in ((1, 0), (2, 1)):
        p_load(i, half).wait()
    for i in (2, 3):
        p_copy(i).wait_send()
    ring_sum(4, 1, 0, add=0)
    ring_sum(5, 2, 1, add=1)

    def send_last():
        @pl.when(core == 1)
        def _():
            for sub in range(C):
                for q in (4, 5):
                    q_part(q, sub).start()

    strips(1, S // 2, S, in_work, send_last)

    for a in range(2):
        for k in range(4):
            ring_own(a, k).wait_send()
        pair_own(a).wait_send()
        for k in (4, 5):
            ring_fwd(a, k).wait_send()
        for k in range(6):
            pair_fwd(a, k).wait_send()
    for q in range(4):
        q_part(q).wait_send()
    for q in (2, 3):
        q_part(q).wait_recv()

    def settle(i, _):
        h = pl.ds(pl.multiple_of(i * 16, 16), 16)
        for q, base in ((3, 0), (2, H)):
            r = pl.ds(pl.multiple_of(base + i * 16, 16), 16)
            acc_v[r] = acc_v[r] + rrecv[q, h].astype(F32)
        return 0

    lax.fori_loop(0, H // 16, settle, 0)

    @pl.when(core == 1)
    def _():
        def finish(sub, _):
            for q, base in ((4, 0), (5, H)):
                q_part(q, sub).wait_recv()

                def put(i, _):
                    h = pl.ds(pl.multiple_of(sub * PIECE + i * 16, 16), 16)
                    r = pl.ds(pl.multiple_of(base + sub * PIECE + i * 16, 16), 16)
                    acc_v[r] = acc_v[r] + rrecv[q, h].astype(F32)
                    return 0

                lax.fori_loop(0, PIECE // 16, put, 0)
            for q in (4, 5):
                q_part(q, sub).wait_send()
            return 0

        lax.fori_loop(0, C, finish, 0)


def last_hop(n, acc_v, last_v, after_ref, dx_ref, recv_v, s_sem, r_sem):
    me = lax.axis_index("tp")
    core = lax.rem(me, 2)
    to = (lax.rem(me + 2, n), lax.rem(me + n - 2, n))
    H = acc_v.shape[0] // 2
    PIECE = H // C

    barrier = pltpu.get_barrier_semaphore()
    for t in to:
        pl.semaphore_signal(barrier, inc=1, device_id={"tp": t}, device_id_type=MESH)
    pl.semaphore_wait(barrier, 2)

    def part(q, sub):
        h = pl.ds(pl.multiple_of(sub * PIECE, PIECE), PIECE)
        return pltpu.make_async_remote_copy(
            src_ref=last_v.at[q, h], dst_ref=recv_v.at[q, h], send_sem=s_sem.at[q, sub], recv_sem=r_sem.at[q, sub],
            device_id={"tp": to[q]}, device_id_type=MESH,
        )

    def finish(lo, count, add):
        for q in range(2):
            def put(i, _):
                h = pl.ds(pl.multiple_of(lo + i * 16, 16), 16)
                r = pl.ds(pl.multiple_of(q * H + lo + i * 16, 16), 16)
                v = acc_v[r]
                if add:
                    v = v + recv_v[q, h].astype(F32)
                dx_ref[r] = v.astype(BF16)
                return 0

            lax.fori_loop(0, count // 16, put, 0)

    @pl.when(core == 0)
    def _():
        for sub in range(C):
            for q in range(2):
                part(q, sub).start()

        def each(sub, _):
            for q in range(2):
                part(q, sub).wait_recv()
            finish(sub * PIECE, PIECE, True)
            for q in range(2):
                part(q, sub).wait_send()
            return 0

        lax.fori_loop(0, C, each, 0)

    @pl.when(core == 1)
    def _():
        finish(0, H, False)


def write_out(*refs):
    k = (len(refs) - 2) // 2
    refs[-2][...] = jnp.zeros_like(refs[-2])
    copies = [pltpu.make_async_copy(refs[i], refs[k + i], refs[-1].at[i]) for i in range(k)]
    for c in copies:
        c.start()
    for c in copies:
        c.wait()


def solution(mesh):
    n = mesh.shape["tp"]

    def body(x, dy, gate, up, w_gate, w_up, w_down):
        R, D = x.shape
        T, F = gate.shape
        H = R // 2
        W = 256
        out = lambda *s: jax.ShapeDtypeStruct(s, BF16)
        vmem_spec = pl.BlockSpec(memory_space=pltpu.VMEM)
        any_spec = pl.BlockSpec(memory_space=pl.ANY)
        dma = pltpu.SemaphoreType.DMA
        vmem = lambda s, t: pltpu.VMEM(s, t)
        keep = lambda a: pltpu.with_memory_space_constraint(a, pltpu.VMEM)

        *dw, acc, last, _, _, _ = pl.pallas_call(
            functools.partial(kernel, n),
            out_shape=[vmem(s, BF16) for s in ((D, F), (D, F), (F, D))]
            + [vmem((R, D), F32), vmem((2, H, D), BF16), out(T, D), out(T, D), out(4, R, D)],
            in_specs=[any_spec] * 7,
            out_specs=[vmem_spec] * 5 + [any_spec] * 3,
            scratch_shapes=[
                pltpu.VMEM((D, 2 * F), BF16),
                pltpu.VMEM((T, 2 * F), BF16),
                pltpu.VMEM((T, F), BF16),
                pltpu.VMEM((2, R, D), BF16),
                pltpu.VMEM((2, 2, R, F), BF16),
                pltpu.VMEM((R, F), F32),
                pltpu.VMEM((2, R, D), BF16),
                pltpu.VMEM((4, H, D), BF16),
                pltpu.VMEM((6, H, D), BF16),
                pltpu.VMEM((2, T, W), BF16),
                dma((2, 13)), dma((2, 13)),
                dma((4,)), dma((4,)),
                dma((4 + 2 * C,)), dma((4 + 2 * C,)),
                dma((3,)), dma((2, 2)), dma((2,)), dma((2,)),
                dma((2,)),
            ],
            compiler_params=pltpu.CompilerParams(collective_id=0, has_side_effects=True, vmem_limit_bytes=199 * 2**18),
            name="mlp_backward",
        )(x, dy, gate, up, w_gate, w_up, w_down)
        *dw, written = pl.pallas_call(
            write_out,
            out_shape=[out(*a.shape) for a in dw] + [vmem((8, 128), F32)],
            in_specs=[vmem_spec] * len(dw),
            out_specs=[any_spec] * len(dw) + [vmem_spec],
            scratch_shapes=[dma((len(dw),))],
            compiler_params=pltpu.CompilerParams(vmem_limit_bytes=2**18),
            name="write_weight_gradients",
        )(*(keep(a) for a in dw))
        dx = pl.pallas_call(
            functools.partial(last_hop, n),
            out_shape=vmem((R, D), BF16),
            in_specs=[vmem_spec] * 3,
            out_specs=vmem_spec,
            scratch_shapes=[pltpu.VMEM((2, H, D), BF16), dma((2, C)), dma((2, C))],
            compiler_params=pltpu.CompilerParams(collective_id=1, has_side_effects=True, vmem_limit_bytes=2**22),
            name="last_hop",
        )(keep(acc), keep(last), keep(written))
        return (dx, *dw)

    tok, col, row = P(("dp", "tp"), None), P("dp", "tp"), P("tp", None)
    wcol = P(None, "tp")
    return jax.shard_map(
        body, mesh=mesh, in_specs=(tok, tok, col, col, wcol, wcol, row), out_specs=(tok, col, col, tok), check_vma=False
    )
```

```python
import functools

import jax
import jax.numpy as jnp
from jax import lax
from jax.experimental import pallas as pl
from jax.experimental.pallas import tpu as pltpu
from jax.sharding import PartitionSpec as P

MESH = pl.DeviceIdType.MESH
BF16, F32 = jnp.bfloat16, jnp.float32
NT = (((1,), (1,)), ((), ()))
TN = (((0,), (0,)), ((), ()))
C = 4


def act(gate, up):
    return jax.nn.gelu(gate) * up


def kernel(
    n, x_ref, dy_ref, gate_ref, up_ref, wg_ref, wu_ref, wd_ref,
    dwg_ref, dwu_ref, dwd_ref, acc_v, last_v, dyg, xg, pbuf,
    wgu_v, dgu_v, hid_v, tile_v, gu_v, dh_v, psend, rsend, rrecv, strip_v,
    side_sem, ag_s, ag_r, p_s, p_r, q_s, q_r, w_sem, g_sem, t_sem, own_sem, st_sem,
):
    me = lax.axis_index("tp")
    core = lax.rem(me, 2)
    other = 1 - 2 * core
    right, left, far = lax.rem(me + 2, n), lax.rem(me + n - 2, n), lax.rem(me + 4, n)
    partner = me + other
    R, D = dy_ref.shape
    H = R // 2
    F = gate_ref.shape[1]
    T = n * R

    def rows(block, half=None):
        if half is None:
            return pl.ds(pl.multiple_of(block * R, R), R)
        return pl.ds(pl.multiple_of(block * R + half * H, H), H)

    def local(src, dst, sem):
        return pltpu.make_async_copy(src, dst, sem)

    def remote(src, dst, s, r, to):
        return pltpu.make_async_remote_copy(src_ref=src, dst_ref=dst, send_sem=s, recv_sem=r, device_id={"tp": to}, device_id_type=MESH)

    pieces = ((left, 0), (left, 1), (right, 1), (right, 0), (far, 0), (far, 1))
    own_sends = ((right, 0), (right, 1), (left, 1), (left, 0))
    own = (dy_ref, x_ref)
    full = (dyg, xg)

    def ring_own(a, k):
        to, half = own_sends[k]
        return remote(own[a].at[pl.ds(half * H, H)], full[a].at[rows(me, half)], ag_s.at[a, k], ag_r.at[a, k], to)

    def ring_fwd(a, k):
        block, half, to = ((left, 0, right), (right, 1, left))[k - 4]
        ref = full[a].at[rows(block, half)]
        return remote(ref, ref, ag_s.at[a, k], ag_r.at[a, k], to)

    def ring_arrived(a, k):
        block, half = pieces[k]
        ref = full[a].at[rows(block, half)]
        remote(ref, ref, ag_s.at[a, k], ag_r.at[a, k], partner).wait_recv()

    def pair_own(a):
        return remote(own[a], full[a].at[rows(me)], ag_s.at[a, 6], ag_r.at[a, 6], partner)

    def pair_fwd(a, k):
        block, half = pieces[k]
        ref = full[a].at[rows(block, half)]
        return remote(ref, ref, ag_s.at[a, 7 + k], ag_r.at[a, 7 + k], partner)

    def pair_arrived(a, k):
        if k < 0:
            ref = full[a].at[rows(partner)]
            remote(ref, ref, ag_s.at[a, 6], ag_r.at[a, 6], partner).wait_recv()
        else:
            block, half = pieces[k]
            ref = full[a].at[rows(block + other, half)]
            remote(ref, ref, ag_s.at[a, 7 + k], ag_r.at[a, 7 + k], partner).wait_recv()

    wd_v = dwd_ref
    w_copies = (
        local(wd_ref, wd_v, w_sem.at[0]),
        local(wg_ref, wgu_v.at[:, pl.ds(0, F)], w_sem.at[1]),
        local(wu_ref, wgu_v.at[:, pl.ds(F, F)], w_sem.at[2]),
    )

    barrier = pltpu.get_barrier_semaphore()
    for to in (left, right):
        pl.semaphore_signal(barrier, inc=1, device_id={"tp": to}, device_id_type=MESH)

    @pl.when(core == 1)
    def _():
        pl.semaphore_signal(barrier, inc=1, device_id={"tp": partner}, device_id_type=MESH)

    pl.semaphore_wait(barrier, 3 - core)

    @pl.when(core == 0)
    def _():
        pl.semaphore_signal(side_sem, inc=1, device_id={"tp": partner}, device_id_type=MESH)

    for k in (0, 2, 1, 3):
        ring_own(0, k).start()

    @pl.when(core == 1)
    def _():
        pl.semaphore_wait(side_sem, 1)

    pair_own(0).start()
    pair_own(1).start()

    def block_of(s):
        j = s // 2
        hop = j + j // 2 - 2 * (j // 3)
        return lax.rem(me + 2 * hop, n) + lax.rem(s, 2) * other

    def gate_load(s, slot):
        r = rows(block_of(s))
        return (
            local(gate_ref.at[r], gu_v.at[slot, 0], g_sem.at[slot, 0]),
            local(up_ref.at[r], gu_v.at[slot, 1], g_sem.at[slot, 1]),
        )

    def tile_load(s, slot):
        return local(dyg.at[rows(block_of(s))], tile_v.at[slot], t_sem.at[slot])

    w_copies[0].start()
    local(dy_ref, tile_v.at[0], t_sem.at[0]).start()
    for c in gate_load(0, 0):
        c.start()
    stage = [local(dy_ref, psend.at[0], own_sem.at[0]), local(x_ref, psend.at[1], own_sem.at[1])]
    for c in stage:
        c.start()
    w_copies[1].start()
    w_copies[2].start()
    keep_own = [local(psend.at[0], dyg.at[rows(me)], own_sem.at[0]), local(psend.at[1], xg.at[rows(me)], own_sem.at[1])]
    w_copies[0].wait()

    def step(s, _):
        slot, nxt = lax.rem(s, 2), lax.rem(s + 1, 2)
        r = rows(block_of(s))
        tile_load(s, slot).wait()
        for c in gate_load(s, slot):
            c.wait()
        dh_v[...] = lax.dot_general(tile_v[slot], wd_v[...], NT, preferred_element_type=F32)

        @pl.when(s == 0)
        def _():
            for c in stage:
                c.wait()
            for c in keep_own:
                c.start()
            pair_arrived(0, -1)

        @pl.when(s == 1)
        def _():
            for k in (0, 2):
                ring_arrived(0, k)
            for k in (4, 5):
                ring_fwd(0, k).start()
            for k in (0, 2, 1, 3):
                ring_own(1, k).start()
            for k in (0, 2):
                pair_fwd(0, k).start()
            for k in (1, 3):
                ring_arrived(0, k)
                pair_fwd(0, k).start()

        @pl.when(s == 2)
        def _():
            for k in (2, 3):
                pair_arrived(0, k)

        @pl.when(s == 4)
        def _():
            for k in (0, 1):
                pair_arrived(0, k)

        @pl.when(s == 5)
        def _():
            for k in (4, 5):
                ring_arrived(0, k)
                pair_fwd(0, k).start()

        @pl.when(s == 6)
        def _():
            for k in (4, 5):
                pair_arrived(0, k)

        @pl.when(s < n - 1)
        def _():
            tile_load(s + 1, nxt).start()
            for c in gate_load(s + 1, nxt):
                c.start()

        def chunk(i, _):
            m = 16
            q = pl.ds(pl.multiple_of(i * m, m), m)
            o = pl.ds(pl.multiple_of(block_of(s) * R + i * m, m), m)
            hidden, back = jax.vjp(act, gu_v[slot, 0, q].astype(F32), gu_v[slot, 1, q].astype(F32))
            dg, du = back(dh_v[q])
            dgu_v[o, pl.ds(0, F)] = dg.astype(BF16)
            dgu_v[o, pl.ds(F, F)] = du.astype(BF16)
            hid_v[o] = hidden.astype(BF16)
            return 0

        lax.fori_loop(0, R // 16, chunk, 0)
        return 0

    lax.fori_loop(0, n, step, 0)
    for c in keep_own:
        c.wait()
    for c in w_copies[1:]:
        c.wait()

    W = strip_v.shape[2]

    def strip_load(a, t, slot):
        return local(full[a].at[:, pl.ds(pl.multiple_of(t * W, W), W)], strip_v.at[slot], st_sem.at[slot])

    NB = 512

    def dx_terms(row0, m, emit):
        def ntile(t, _):
            cols = pl.ds(pl.multiple_of(t * NB, NB), NB)
            emit(cols, lax.dot_general(dgu_v[pl.ds(row0, m)], wgu_v[cols], NT, preferred_element_type=F32))
            return 0

        lax.fori_loop(0, D // NB, ntile, 0)

    targets = (far, right, left, me)

    def p_copy(i):
        return remote(psend.at[i % 2], pbuf.at[i], p_s.at[i], p_r.at[i], partner)

    for i, block in enumerate(targets):
        if i >= 2:
            p_copy(i - 2).wait_send()

        def emit(cols, v, i=i):
            psend[i % 2, :, cols] = v.astype(BF16)

        dx_terms(pl.multiple_of((block + other) * R, R), R, emit)
        if i >= 1:
            p_copy(i - 1).start()

    for k in (0, 2):
        ring_arrived(1, k)
    for k in (4, 5):
        ring_fwd(1, k).start()
    for k in (0, 2):
        pair_fwd(1, k).start()
    p_copy(3).start()

    def p_load(i, half=None):
        if half is None:
            return local(pbuf.at[i], tile_v.at[i % 2], t_sem.at[i % 2])
        h = pl.ds(half * H, H)
        return local(pbuf.at[i, h], tile_v.at[i % 2, h], t_sem.at[i % 2])

    def p_fetch(i):
        p_copy(i).wait_recv()
        p_load(i).start()

    PIECE = H // C

    def q_src(q):
        return rsend.at[q] if q < 4 else last_v.at[q - 4]

    def q_part(q, sub=None):
        h, k = (pl.ds(0, H), q) if sub is None else (pl.ds(pl.multiple_of(sub * PIECE, PIECE), PIECE), q + 2 * sub)
        return remote(q_src(q).at[h], rrecv.at[q, h], q_s.at[k], q_r.at[k], (right, left)[q % 2])

    def q_parts(q):
        return [q_part(q)] if q < 4 else [q_part(q, sub) for sub in range(C)]

    def ring_sum(q, i, half, add=None):
        h = pl.ds(half * H, H)
        dst = q_src(q)

        def emit(cols, v):
            v = v + tile_v[i % 2, h, cols].astype(F32)
            if add is not None:
                v = v + rrecv[add, :, cols].astype(F32)
            dst[:, cols] = v.astype(BF16)

        dx_terms(pl.multiple_of(targets[i] * R + half * H, H), H, emit)
        if 1 <= q < 4:
            q_part(q - 1).start()

    p_fetch(0)
    p_fetch(1)
    p_load(0).wait()
    ring_sum(0, 0, 0)
    ring_sum(1, 0, 1)
    p_fetch(2)
    p_load(1).wait()
    ring_sum(2, 1, 1)
    p_fetch(3)
    p_load(2).wait()
    ring_sum(3, 2, 0)
    p_load(3).wait()

    def emit_own(cols, v):
        acc_v[:, cols] = v + tile_v[1, :, cols].astype(F32)

    strip_load(0, 0, 0).start()
    dx_terms(pl.multiple_of(me * R, R), R, emit_own)
    q_part(3).start()

    for k in (1, 3):
        ring_arrived(1, k)
        pair_fwd(1, k).start()

    def strips(a, lo, hi, work, after_first=lambda: None):
        def one(t, _):
            slot = lax.rem(t, 2)
            strip_load(a, t, slot).wait()

            @pl.when(t + 1 < hi)
            def _():
                strip_load(a, t + 1, 1 - slot).start()

            work(slot, pl.ds(pl.multiple_of(t * W, W), W))
            pl.when(t == lo)(after_first)
            return 0

        lax.fori_loop(lo, hi, one, 0)

    def down_work(slot, part):
        v = lax.dot_general(strip_v[slot], hid_v[...], TN, preferred_element_type=F32)
        dwd_ref[:, part] = v.T.astype(BF16)

    def in_work(slot, part):
        v = lax.dot_general(strip_v[slot], dgu_v[...], TN, preferred_element_type=F32)
        dwg_ref[part] = v[:, :F].astype(BF16)
        dwu_ref[part] = v[:, F:].astype(BF16)

    S = D // W
    strips(0, 0, S, down_work)

    for k in (4, 5):
        ring_arrived(1, k)
        pair_fwd(1, k).start()
    for k in (-1, 0, 1, 2, 3, 4, 5):
        pair_arrived(1, k)

    strip_load(1, 0, 0).start()
    for i, half in ((1, 0), (2, 1)):
        p_load(i, half).start()
    strips(1, 0, S // 2, in_work)

    strip_load(1, S // 2, S // 2 % 2).start()
    for c in q_parts(0) + q_parts(1):
        c.wait_recv()
    for i, half in ((1, 0), (2, 1)):
        p_load(i, half).wait()
    for i in (2, 3):
        p_copy(i).wait_send()
    ring_sum(4, 1, 0, add=0)
    ring_sum(5, 2, 1, add=1)

    def send_last():
        @pl.when(core == 1)
        def _():
            for sub in range(C):
                for q in (4, 5):
                    q_part(q, sub).start()

    strips(1, S // 2, S, in_work, send_last)

    for a in range(2):
        for k in range(4):
            ring_own(a, k).wait_send()
        pair_own(a).wait_send()
        for k in (4, 5):
            ring_fwd(a, k).wait_send()
        for k in range(6):
            pair_fwd(a, k).wait_send()
    for q in range(4):
        q_part(q).wait_send()
    for q in (2, 3):
        q_part(q).wait_recv()

    def settle(i, _):
        h = pl.ds(pl.multiple_of(i * 16, 16), 16)
        for q, base in ((3, 0), (2, H)):
            r = pl.ds(pl.multiple_of(base + i * 16, 16), 16)
            acc_v[r] = acc_v[r] + rrecv[q, h].astype(F32)
        return 0

    lax.fori_loop(0, H // 16, settle, 0)

    @pl.when(core == 1)
    def _():
        def finish(sub, _):
            for q, base in ((4, 0), (5, H)):
                q_part(q, sub).wait_recv()

                def put(i, _):
                    h = pl.ds(pl.multiple_of(sub * PIECE + i * 16, 16), 16)
                    r = pl.ds(pl.multiple_of(base + sub * PIECE + i * 16, 16), 16)
                    acc_v[r] = acc_v[r] + rrecv[q, h].astype(F32)
                    return 0

                lax.fori_loop(0, PIECE // 16, put, 0)
            for q in (4, 5):
                q_part(q, sub).wait_send()
            return 0

        lax.fori_loop(0, C, finish, 0)


def last_hop(n, acc_v, last_v, after_ref, dx_ref, recv_v, s_sem, r_sem):
    me = lax.axis_index("tp")
    core = lax.rem(me, 2)
    to = (lax.rem(me + 2, n), lax.rem(me + n - 2, n))
    H = acc_v.shape[0] // 2
    PIECE = H // C

    barrier = pltpu.get_barrier_semaphore()
    for t in to:
        pl.semaphore_signal(barrier, inc=1, device_id={"tp": t}, device_id_type=MESH)
    pl.semaphore_wait(barrier, 2)

    def part(q, sub):
        h = pl.ds(pl.multiple_of(sub * PIECE, PIECE), PIECE)
        return pltpu.make_async_remote_copy(
            src_ref=last_v.at[q, h], dst_ref=recv_v.at[q, h], send_sem=s_sem.at[q, sub], recv_sem=r_sem.at[q, sub],
            device_id={"tp": to[q]}, device_id_type=MESH,
        )

    def finish(lo, count, add):
        for q in range(2):
            def put(i, _):
                h = pl.ds(pl.multiple_of(lo + i * 16, 16), 16)
                r = pl.ds(pl.multiple_of(q * H + lo + i * 16, 16), 16)
                v = acc_v[r]
                if add:
                    v = v + recv_v[q, h].astype(F32)
                dx_ref[r] = v.astype(BF16)
                return 0

            lax.fori_loop(0, count // 16, put, 0)

    @pl.when(core == 0)
    def _():
        for sub in range(C):
            for q in range(2):
                part(q, sub).start()

        def each(sub, _):
            for q in range(2):
                part(q, sub).wait_recv()
            finish(sub * PIECE, PIECE, True)
            for q in range(2):
                part(q, sub).wait_send()
            return 0

        lax.fori_loop(0, C, each, 0)

    @pl.when(core == 1)
    def _():
        finish(0, H, False)


def write_out(*refs):
    k = (len(refs) - 2) // 2
    refs[-2][...] = jnp.zeros_like(refs[-2])
    copies = [pltpu.make_async_copy(refs[i], refs[k + i], refs[-1].at[i]) for i in range(k)]
    for c in copies:
        c.start()
    for c in copies:
        c.wait()


def solution(mesh):
    n = mesh.shape["tp"]

    def body(x, dy, gate, up, w_gate, w_up, w_down):
        R, D = x.shape
        T, F = gate.shape
        H = R // 2
        W = 256
        out = lambda *s: jax.ShapeDtypeStruct(s, BF16)
        vmem_spec = pl.BlockSpec(memory_space=pltpu.VMEM)
        any_spec = pl.BlockSpec(memory_space=pl.ANY)
        dma = pltpu.SemaphoreType.DMA
        vmem = lambda s, t: pltpu.VMEM(s, t)
        keep = lambda a: pltpu.with_memory_space_constraint(a, pltpu.VMEM)

        *dw, acc, last, _, _, _ = pl.pallas_call(
            functools.partial(kernel, n),
            out_shape=[vmem(s, BF16) for s in ((D, F), (D, F), (F, D))]
            + [vmem((R, D), F32), vmem((2, H, D), BF16), out(T, D), out(T, D), out(4, R, D)],
            in_specs=[any_spec] * 7,
            out_specs=[vmem_spec] * 5 + [any_spec] * 3,
            scratch_shapes=[
                pltpu.VMEM((D, 2 * F), BF16),
                pltpu.VMEM((T, 2 * F), BF16),
                pltpu.VMEM((T, F), BF16),
                pltpu.VMEM((2, R, D), BF16),
                pltpu.VMEM((2, 2, R, F), BF16),
                pltpu.VMEM((R, F), F32),
                pltpu.VMEM((2, R, D), BF16),
                pltpu.VMEM((4, H, D), BF16),
                pltpu.VMEM((6, H, D), BF16),
                pltpu.VMEM((2, T, W), BF16),
                pltpu.SemaphoreType.REGULAR,
                dma((2, 13)), dma((2, 13)),
                dma((4,)), dma((4,)),
                dma((4 + 2 * C,)), dma((4 + 2 * C,)),
                dma((3,)), dma((2, 2)), dma((2,)), dma((2,)),
                dma((2,)),
            ],
            compiler_params=pltpu.CompilerParams(collective_id=0, has_side_effects=True, vmem_limit_bytes=199 * 2**18),
            name="mlp_backward",
        )(x, dy, gate, up, w_gate, w_up, w_down)
        *dw, written = pl.pallas_call(
            write_out,
            out_shape=[out(*a.shape) for a in dw] + [vmem((8, 128), F32)],
            in_specs=[vmem_spec] * len(dw),
            out_specs=[any_spec] * len(dw) + [vmem_spec],
            scratch_shapes=[dma((len(dw),))],
            compiler_params=pltpu.CompilerParams(vmem_limit_bytes=2**18),
            name="write_weight_gradients",
        )(*(keep(a) for a in dw))
        dx = pl.pallas_call(
            functools.partial(last_hop, n),
            out_shape=vmem((R, D), BF16),
            in_specs=[vmem_spec] * 3,
            out_specs=vmem_spec,
            scratch_shapes=[pltpu.VMEM((2, H, D), BF16), dma((2, C)), dma((2, C))],
            compiler_params=pltpu.CompilerParams(collective_id=1, has_side_effects=True, vmem_limit_bytes=2**22),
            name="last_hop",
        )(keep(acc), keep(last), keep(written))
        return (dx, *dw)

    tok, col, row = P(("dp", "tp"), None), P("dp", "tp"), P("tp", None)
    wcol = P(None, "tp")
    return jax.shard_map(
        body, mesh=mesh, in_specs=(tok, tok, col, col, wcol, wcol, row), out_specs=(tok, col, col, tok), check_vma=False
    )
```

```python
import functools

import jax
import jax.numpy as jnp
from jax import lax
from jax.experimental import pallas as pl
from jax.experimental.pallas import tpu as pltpu
from jax.sharding import PartitionSpec as P

MESH = pl.DeviceIdType.MESH
BF16, F32 = jnp.bfloat16, jnp.float32
NT = (((1,), (1,)), ((), ()))
TN = (((0,), (0,)), ((), ()))
C = 4


def act(gate, up):
    return jax.nn.gelu(gate) * up


def kernel(
    n, x_ref, dy_ref, gate_ref, up_ref, wg_ref, wu_ref, wd_ref,
    dwg_ref, dwu_ref, dwd_ref, acc_v, last_v, dyg, xg, pbuf,
    wgu_v, dgu_v, hid_v, tile_v, gu_v, dh_v, psend, rsend, rrecv, strip_v,
    side_sem, ag_s, ag_r, p_s, p_r, q_s, q_r, w_sem, g_sem, t_sem, own_sem, st_sem,
):
    me = lax.axis_index("tp")
    core = lax.rem(me, 2)
    other = 1 - 2 * core
    right, left, far = lax.rem(me + 2, n), lax.rem(me + n - 2, n), lax.rem(me + 4, n)
    partner = me + other
    R, D = dy_ref.shape
    H = R // 2
    F = gate_ref.shape[1]
    T = n * R

    def rows(block, half=None):
        if half is None:
            return pl.ds(pl.multiple_of(block * R, R), R)
        return pl.ds(pl.multiple_of(block * R + half * H, H), H)

    def local(src, dst, sem):
        return pltpu.make_async_copy(src, dst, sem)

    def remote(src, dst, s, r, to):
        return pltpu.make_async_remote_copy(src_ref=src, dst_ref=dst, send_sem=s, recv_sem=r, device_id={"tp": to}, device_id_type=MESH)

    pieces = ((left, 0), (left, 1), (right, 1), (right, 0), (far, 0), (far, 1))
    own_sends = ((right, 0), (right, 1), (left, 1), (left, 0))
    own = (dy_ref, x_ref)
    full = (dyg, xg)

    def ring_own(a, k):
        to, half = own_sends[k]
        return remote(own[a].at[pl.ds(half * H, H)], full[a].at[rows(me, half)], ag_s.at[a, k], ag_r.at[a, k], to)

    def ring_fwd(a, k):
        block, half, to = ((left, 0, right), (right, 1, left))[k - 4]
        ref = full[a].at[rows(block, half)]
        return remote(ref, ref, ag_s.at[a, k], ag_r.at[a, k], to)

    def ring_arrived(a, k):
        block, half = pieces[k]
        ref = full[a].at[rows(block, half)]
        remote(ref, ref, ag_s.at[a, k], ag_r.at[a, k], partner).wait_recv()

    def pair_own(a):
        return remote(own[a], full[a].at[rows(me)], ag_s.at[a, 6], ag_r.at[a, 6], partner)

    def pair_fwd(a, k):
        block, half = pieces[k]
        ref = full[a].at[rows(block, half)]
        return remote(ref, ref, ag_s.at[a, 7 + k], ag_r.at[a, 7 + k], partner)

    def pair_arrived(a, k):
        if k < 0:
            ref = full[a].at[rows(partner)]
            remote(ref, ref, ag_s.at[a, 6], ag_r.at[a, 6], partner).wait_recv()
        else:
            block, half = pieces[k]
            ref = full[a].at[rows(block + other, half)]
            remote(ref, ref, ag_s.at[a, 7 + k], ag_r.at[a, 7 + k], partner).wait_recv()

    wd_v = dwd_ref
    w_copies = (
        local(wd_ref, wd_v, w_sem.at[0]),
        local(wg_ref, wgu_v.at[:, pl.ds(0, F)], w_sem.at[1]),
        local(wu_ref, wgu_v.at[:, pl.ds(F, F)], w_sem.at[2]),
    )

    barrier = pltpu.get_barrier_semaphore()
    for to in (left, right):
        pl.semaphore_signal(barrier, inc=1, device_id={"tp": to}, device_id_type=MESH)

    @pl.when(core == 1)
    def _():
        pl.semaphore_signal(barrier, inc=1, device_id={"tp": partner}, device_id_type=MESH)

    pl.semaphore_wait(barrier, 3 - core)

    @pl.when(core == 0)
    def _():
        pl.semaphore_signal(side_sem, inc=1, device_id={"tp": partner}, device_id_type=MESH)

    for k in (0, 2, 1, 3):
        ring_own(0, k).start()

    @pl.when(core == 1)
    def _():
        pl.semaphore_wait(side_sem, 1)

    pair_own(0).start()
    pair_own(1).start()

    def block_of(s):
        j = s // 2
        hop = j + j // 2 - 2 * (j // 3)
        return lax.rem(me + 2 * hop, n) + lax.rem(s, 2) * other

    def gate_load(s, slot):
        r = rows(block_of(s))
        return (
            local(gate_ref.at[r], gu_v.at[slot, 0], g_sem.at[slot, 0]),
            local(up_ref.at[r], gu_v.at[slot, 1], g_sem.at[slot, 1]),
        )

    def tile_load(s, slot):
        return local(dyg.at[rows(block_of(s))], tile_v.at[slot], t_sem.at[slot])

    w_copies[0].start()
    local(dy_ref, tile_v.at[0], t_sem.at[0]).start()
    for c in gate_load(0, 0):
        c.start()
    stage = [local(dy_ref, psend.at[0], own_sem.at[0]), local(x_ref, psend.at[1], own_sem.at[1])]
    for c in stage:
        c.start()
    w_copies[1].start()
    w_copies[2].start()
    keep_own = [local(psend.at[0], dyg.at[rows(me)], own_sem.at[0]), local(psend.at[1], xg.at[rows(me)], own_sem.at[1])]
    w_copies[0].wait()

    def step(s, _):
        slot, nxt = lax.rem(s, 2), lax.rem(s + 1, 2)
        r = rows(block_of(s))
        tile_load(s, slot).wait()
        for c in gate_load(s, slot):
            c.wait()
        dh_v[...] = lax.dot_general(tile_v[slot], wd_v[...], NT, preferred_element_type=F32)

        @pl.when(s == 0)
        def _():
            for c in stage:
                c.wait()
            for c in keep_own:
                c.start()
            pair_arrived(0, -1)

        @pl.when(s == 1)
        def _():
            for k in (0, 2):
                ring_arrived(0, k)
            for k in (4, 5):
                ring_fwd(0, k).start()
            for k in (0, 2, 1, 3):
                ring_own(1, k).start()
            for k in (0, 2):
                pair_fwd(0, k).start()
            for k in (1, 3):
                ring_arrived(0, k)
                pair_fwd(0, k).start()

        @pl.when(s == 2)
        def _():
            for k in (2, 3):
                pair_arrived(0, k)

        @pl.when(s == 4)
        def _():
            for k in (0, 1):
                pair_arrived(0, k)

        @pl.when(s == 5)
        def _():
            for k in (4, 5):
                ring_arrived(0, k)
                pair_fwd(0, k).start()

        @pl.when(s == 6)
        def _():
            for k in (4, 5):
                pair_arrived(0, k)

        @pl.when(s < n - 1)
        def _():
            tile_load(s + 1, nxt).start()
            for c in gate_load(s + 1, nxt):
                c.start()

        def chunk(i, _):
            m = 16
            q = pl.ds(pl.multiple_of(i * m, m), m)
            o = pl.ds(pl.multiple_of(block_of(s) * R + i * m, m), m)
            hidden, back = jax.vjp(act, gu_v[slot, 0, q].astype(F32), gu_v[slot, 1, q].astype(F32))
            dg, du = back(dh_v[q])
            dgu_v[o, pl.ds(0, F)] = dg.astype(BF16)
            dgu_v[o, pl.ds(F, F)] = du.astype(BF16)
            hid_v[o] = hidden.astype(BF16)
            return 0

        lax.fori_loop(0, R // 16, chunk, 0)
        return 0

    lax.fori_loop(0, n, step, 0)
    for c in keep_own:
        c.wait()
    for c in w_copies[1:]:
        c.wait()

    W = strip_v.shape[2]

    def strip_load(a, t, slot):
        return local(full[a].at[:, pl.ds(pl.multiple_of(t * W, W), W)], strip_v.at[slot], st_sem.at[slot])

    NB = 512

    def dx_terms(row0, m, emit):
        def ntile(t, _):
            cols = pl.ds(pl.multiple_of(t * NB, NB), NB)
            emit(cols, lax.dot_general(dgu_v[pl.ds(row0, m)], wgu_v[cols], NT, preferred_element_type=F32))
            return 0

        lax.fori_loop(0, D // NB, ntile, 0)

    targets = (far, right, left, me)

    def p_copy(i):
        return remote(psend.at[i % 2], pbuf.at[i], p_s.at[i], p_r.at[i], partner)

    for i, block in enumerate(targets):
        if i >= 2:
            p_copy(i - 2).wait_send()

        def emit(cols, v, i=i):
            psend[i % 2, :, cols] = v.astype(BF16)

        dx_terms(pl.multiple_of((block + other) * R, R), R, emit)
        if i >= 1:
            p_copy(i - 1).start()

    def p_load(i, half=None):
        if half is None:
            return local(pbuf.at[i], tile_v.at[i % 2], t_sem.at[i % 2])
        h = pl.ds(half * H, H)
        return local(pbuf.at[i, h], tile_v.at[i % 2, h], t_sem.at[i % 2])

    def p_fetch(i):
        p_copy(i).wait_recv()
        p_load(i).start()

    PIECE = H // C

    def q_src(q):
        return rsend.at[q] if q < 4 else last_v.at[q - 4]

    def q_part(q, sub=None):
        h, k = (pl.ds(0, H), q) if sub is None else (pl.ds(pl.multiple_of(sub * PIECE, PIECE), PIECE), q + 2 * sub)
        return remote(q_src(q).at[h], rrecv.at[q, h], q_s.at[k], q_r.at[k], (right, left)[q % 2])

    def q_parts(q):
        return [q_part(q)] if q < 4 else [q_part(q, sub) for sub in range(C)]

    def ring_sum(q, i, half, add=None):
        h = pl.ds(half * H, H)
        dst = q_src(q)

        def emit(cols, v):
            v = v + tile_v[i % 2, h, cols].astype(F32)
            if add is not None:
                v = v + rrecv[add, :, cols].astype(F32)
            dst[:, cols] = v.astype(BF16)

        dx_terms(pl.multiple_of(targets[i] * R + half * H, H), H, emit)
        if 1 <= q < 4:
            q_part(q - 1).start()

    p_fetch(0)
    p_fetch(1)

    for k in (0, 2):
        ring_arrived(1, k)
    for k in (4, 5):
        ring_fwd(1, k).start()
    for k in (0, 2):
        pair_fwd(1, k).start()
    p_copy(3).start()

    p_load(0).wait()
    ring_sum(0, 0, 0)
    ring_sum(1, 0, 1)
    p_fetch(2)
    p_load(1).wait()
    ring_sum(2, 1, 1)
    p_fetch(3)
    p_load(2).wait()
    ring_sum(3, 2, 0)
    p_load(3).wait()

    def emit_own(cols, v):
        acc_v[:, cols] = v + tile_v[1, :, cols].astype(F32)

    strip_load(0, 0, 0).start()
    dx_terms(pl.multiple_of(me * R, R), R, emit_own)
    q_part(3).start()

    for k in (1, 3):
        ring_arrived(1, k)
        pair_fwd(1, k).start()

    def strips(a, lo, hi, work, after_first=lambda: None, before_last=lambda: None):
        def one(t, _):
            slot = lax.rem(t, 2)
            strip_load(a, t, slot).wait()

            @pl.when(t + 1 < hi)
            def _():
                strip_load(a, t + 1, 1 - slot).start()

            pl.when(t + 1 == hi)(before_last)
            work(slot, pl.ds(pl.multiple_of(t * W, W), W))
            pl.when(t == lo)(after_first)
            return 0

        lax.fori_loop(lo, hi, one, 0)

    def down_work(slot, part):
        v = lax.dot_general(strip_v[slot], hid_v[...], TN, preferred_element_type=F32)
        dwd_ref[:, part] = v.T.astype(BF16)

    def in_work(slot, part):
        v = lax.dot_general(strip_v[slot], dgu_v[...], TN, preferred_element_type=F32)
        dwg_ref[part] = v[:, :F].astype(BF16)
        dwu_ref[part] = v[:, F:].astype(BF16)

    S = D // W
    def x_complete():
        for k in (4, 5):
            ring_arrived(1, k)
            pair_fwd(1, k).start()
        for k in (-1, 0, 1, 2, 3, 4, 5):
            pair_arrived(1, k)
        strip_load(1, 0, 0).start()

    strips(0, 0, S, down_work, before_last=x_complete)

    for i, half in ((1, 0), (2, 1)):
        p_load(i, half).start()
    strips(1, 0, S // 2, in_work)

    strip_load(1, S // 2, S // 2 % 2).start()
    for c in q_parts(0) + q_parts(1):
        c.wait_recv()
    for i, half in ((1, 0), (2, 1)):
        p_load(i, half).wait()
    for i in (2, 3):
        p_copy(i).wait_send()
    ring_sum(4, 1, 0, add=0)
    ring_sum(5, 2, 1, add=1)

    def send_last():
        @pl.when(core == 1)
        def _():
            for sub in range(C):
                for q in (4, 5):
                    q_part(q, sub).start()

    strips(1, S // 2, S, in_work, send_last)

    for a in range(2):
        for k in range(4):
            ring_own(a, k).wait_send()
        pair_own(a).wait_send()
        for k in (4, 5):
            ring_fwd(a, k).wait_send()
        for k in range(6):
            pair_fwd(a, k).wait_send()
    for q in range(4):
        q_part(q).wait_send()
    for q in (2, 3):
        q_part(q).wait_recv()

    def settle(i, _):
        h = pl.ds(pl.multiple_of(i * 16, 16), 16)
        for q, base in ((3, 0), (2, H)):
            r = pl.ds(pl.multiple_of(base + i * 16, 16), 16)
            acc_v[r] = acc_v[r] + rrecv[q, h].astype(F32)
        return 0

    lax.fori_loop(0, H // 16, settle, 0)

    @pl.when(core == 1)
    def _():
        def finish(sub, _):
            for q, base in ((4, 0), (5, H)):
                q_part(q, sub).wait_recv()

                def put(i, _):
                    h = pl.ds(pl.multiple_of(sub * PIECE + i * 16, 16), 16)
                    r = pl.ds(pl.multiple_of(base + sub * PIECE + i * 16, 16), 16)
                    acc_v[r] = acc_v[r] + rrecv[q, h].astype(F32)
                    return 0

                lax.fori_loop(0, PIECE // 16, put, 0)
            for q in (4, 5):
                q_part(q, sub).wait_send()
            return 0

        lax.fori_loop(0, C, finish, 0)


def last_hop(n, acc_v, last_v, after_ref, dx_ref, recv_v, s_sem, r_sem):
    me = lax.axis_index("tp")
    core = lax.rem(me, 2)
    to = (lax.rem(me + 2, n), lax.rem(me + n - 2, n))
    H = acc_v.shape[0] // 2
    PIECE = H // C

    barrier = pltpu.get_barrier_semaphore()
    for t in to:
        pl.semaphore_signal(barrier, inc=1, device_id={"tp": t}, device_id_type=MESH)
    pl.semaphore_wait(barrier, 2)

    def part(q, sub):
        h = pl.ds(pl.multiple_of(sub * PIECE, PIECE), PIECE)
        return pltpu.make_async_remote_copy(
            src_ref=last_v.at[q, h], dst_ref=recv_v.at[q, h], send_sem=s_sem.at[q, sub], recv_sem=r_sem.at[q, sub],
            device_id={"tp": to[q]}, device_id_type=MESH,
        )

    def finish(lo, count, add):
        for q in range(2):
            def put(i, _):
                h = pl.ds(pl.multiple_of(lo + i * 16, 16), 16)
                r = pl.ds(pl.multiple_of(q * H + lo + i * 16, 16), 16)
                v = acc_v[r]
                if add:
                    v = v + recv_v[q, h].astype(F32)
                dx_ref[r] = v.astype(BF16)
                return 0

            lax.fori_loop(0, count // 16, put, 0)

    @pl.when(core == 0)
    def _():
        for sub in range(C):
            for q in range(2):
                part(q, sub).start()

        def each(sub, _):
            for q in range(2):
                part(q, sub).wait_recv()
            finish(sub * PIECE, PIECE, True)
            for q in range(2):
                part(q, sub).wait_send()
            return 0

        lax.fori_loop(0, C, each, 0)

    @pl.when(core == 1)
    def _():
        finish(0, H, False)


def write_out(*refs):
    k = (len(refs) - 2) // 2
    refs[-2][...] = jnp.zeros_like(refs[-2])
    copies = [pltpu.make_async_copy(refs[i], refs[k + i], refs[-1].at[i]) for i in range(k)]
    for c in copies:
        c.start()
    for c in copies:
        c.wait()


def solution(mesh):
    n = mesh.shape["tp"]

    def body(x, dy, gate, up, w_gate, w_up, w_down):
        R, D = x.shape
        T, F = gate.shape
        H = R // 2
        W = 256
        out = lambda *s: jax.ShapeDtypeStruct(s, BF16)
        vmem_spec = pl.BlockSpec(memory_space=pltpu.VMEM)
        any_spec = pl.BlockSpec(memory_space=pl.ANY)
        dma = pltpu.SemaphoreType.DMA
        vmem = lambda s, t: pltpu.VMEM(s, t)
        keep = lambda a: pltpu.with_memory_space_constraint(a, pltpu.VMEM)

        *dw, acc, last, _, _, _ = pl.pallas_call(
            functools.partial(kernel, n),
            out_shape=[vmem(s, BF16) for s in ((D, F), (D, F), (F, D))]
            + [vmem((R, D), F32), vmem((2, H, D), BF16), out(T, D), out(T, D), out(4, R, D)],
            in_specs=[any_spec] * 7,
            out_specs=[vmem_spec] * 5 + [any_spec] * 3,
            scratch_shapes=[
                pltpu.VMEM((D, 2 * F), BF16),
                pltpu.VMEM((T, 2 * F), BF16),
                pltpu.VMEM((T, F), BF16),
                pltpu.VMEM((2, R, D), BF16),
                pltpu.VMEM((2, 2, R, F), BF16),
                pltpu.VMEM((R, F), F32),
                pltpu.VMEM((2, R, D), BF16),
                pltpu.VMEM((4, H, D), BF16),
                pltpu.VMEM((6, H, D), BF16),
                pltpu.VMEM((2, T, W), BF16),
                pltpu.SemaphoreType.REGULAR,
                dma((2, 13)), dma((2, 13)),
                dma((4,)), dma((4,)),
                dma((4 + 2 * C,)), dma((4 + 2 * C,)),
                dma((3,)), dma((2, 2)), dma((2,)), dma((2,)),
                dma((2,)),
            ],
            compiler_params=pltpu.CompilerParams(collective_id=0, has_side_effects=True, vmem_limit_bytes=199 * 2**18),
            name="mlp_backward",
        )(x, dy, gate, up, w_gate, w_up, w_down)
        *dw, written = pl.pallas_call(
            write_out,
            out_shape=[out(*a.shape) for a in dw] + [vmem((8, 128), F32)],
            in_specs=[vmem_spec] * len(dw),
            out_specs=[any_spec] * len(dw) + [vmem_spec],
            scratch_shapes=[dma((len(dw),))],
            compiler_params=pltpu.CompilerParams(vmem_limit_bytes=2**18),
            name="write_weight_gradients",
        )(*(keep(a) for a in dw))
        dx = pl.pallas_call(
            functools.partial(last_hop, n),
            out_shape=vmem((R, D), BF16),
            in_specs=[vmem_spec] * 3,
            out_specs=vmem_spec,
            scratch_shapes=[pltpu.VMEM((2, H, D), BF16), dma((2, C)), dma((2, C))],
            compiler_params=pltpu.CompilerParams(collective_id=1, has_side_effects=True, vmem_limit_bytes=2**22),
            name="last_hop",
        )(keep(acc), keep(last), keep(written))
        return (dx, *dw)

    tok, col, row = P(("dp", "tp"), None), P("dp", "tp"), P("tp", None)
    wcol = P(None, "tp")
    return jax.shard_map(
        body, mesh=mesh, in_specs=(tok, tok, col, col, wcol, wcol, row), out_specs=(tok, col, col, tok), check_vma=False
    )
```

```python
import functools

import jax
import jax.numpy as jnp
from jax import lax
from jax.experimental import pallas as pl
from jax.experimental.pallas import tpu as pltpu
from jax.sharding import PartitionSpec as P

MESH = pl.DeviceIdType.MESH
BF16, F32 = jnp.bfloat16, jnp.float32
NT = (((1,), (1,)), ((), ()))
TN = (((0,), (0,)), ((), ()))
C = 4


def act(gate, up):
    return jax.nn.gelu(gate) * up


def kernel(
    n, x_ref, dy_ref, gate_ref, up_ref, wg_ref, wu_ref, wd_ref,
    dwg_ref, dwu_ref, dwd_ref, acc_v, last_v, dyg, xg, pbuf,
    wgu_v, dgu_v, hid_v, tile_v, gu_v, dh_v, psend, rsend, rrecv, strip_v,
    side_sem, ag_s, ag_r, p_s, p_r, q_s, q_r, w_sem, g_sem, t_sem, own_sem, st_sem,
):
    me = lax.axis_index("tp")
    core = lax.rem(me, 2)
    other = 1 - 2 * core
    right, left, far = lax.rem(me + 2, n), lax.rem(me + n - 2, n), lax.rem(me + 4, n)
    partner = me + other
    R, D = dy_ref.shape
    H = R // 2
    F = gate_ref.shape[1]
    T = n * R

    def rows(block, half=None):
        if half is None:
            return pl.ds(pl.multiple_of(block * R, R), R)
        return pl.ds(pl.multiple_of(block * R + half * H, H), H)

    def local(src, dst, sem):
        return pltpu.make_async_copy(src, dst, sem)

    def remote(src, dst, s, r, to):
        return pltpu.make_async_remote_copy(src_ref=src, dst_ref=dst, send_sem=s, recv_sem=r, device_id={"tp": to}, device_id_type=MESH)

    pieces = ((left, 0), (left, 1), (right, 1), (right, 0), (far, 0), (far, 1))
    own_sends = ((right, 0), (right, 1), (left, 1), (left, 0))
    own = (dy_ref, x_ref)
    full = (dyg, xg)

    def ring_own(a, k):
        to, half = own_sends[k]
        return remote(own[a].at[pl.ds(half * H, H)], full[a].at[rows(me, half)], ag_s.at[a, k], ag_r.at[a, k], to)

    def ring_fwd(a, k):
        block, half, to = ((left, 0, right), (right, 1, left))[k - 4]
        ref = full[a].at[rows(block, half)]
        return remote(ref, ref, ag_s.at[a, k], ag_r.at[a, k], to)

    def ring_arrived(a, k):
        block, half = pieces[k]
        ref = full[a].at[rows(block, half)]
        remote(ref, ref, ag_s.at[a, k], ag_r.at[a, k], partner).wait_recv()

    def pair_own(a):
        return remote(own[a], full[a].at[rows(me)], ag_s.at[a, 6], ag_r.at[a, 6], partner)

    def pair_fwd(a, k):
        block, half = pieces[k]
        ref = full[a].at[rows(block, half)]
        return remote(ref, ref, ag_s.at[a, 7 + k], ag_r.at[a, 7 + k], partner)

    def pair_arrived(a, k):
        if k < 0:
            ref = full[a].at[rows(partner)]
            remote(ref, ref, ag_s.at[a, 6], ag_r.at[a, 6], partner).wait_recv()
        else:
            block, half = pieces[k]
            ref = full[a].at[rows(block + other, half)]
            remote(ref, ref, ag_s.at[a, 7 + k], ag_r.at[a, 7 + k], partner).wait_recv()

    wd_v = dwd_ref
    w_copies = (
        local(wd_ref, wd_v, w_sem.at[0]),
        local(wg_ref, wgu_v.at[:, pl.ds(0, F)], w_sem.at[1]),
        local(wu_ref, wgu_v.at[:, pl.ds(F, F)], w_sem.at[2]),
    )

    barrier = pltpu.get_barrier_semaphore()
    for to in (left, right):
        pl.semaphore_signal(barrier, inc=1, device_id={"tp": to}, device_id_type=MESH)

    @pl.when(core == 1)
    def _():
        pl.semaphore_signal(barrier, inc=1, device_id={"tp": partner}, device_id_type=MESH)

    pl.semaphore_wait(barrier, 3 - core)

    @pl.when(core == 0)
    def _():
        pl.semaphore_signal(side_sem, inc=1, device_id={"tp": partner}, device_id_type=MESH)

    for k in (0, 2, 1, 3):
        ring_own(0, k).start()

    @pl.when(core == 1)
    def _():
        pl.semaphore_wait(side_sem, 1)

    pair_own(0).start()
    pair_own(1).start()

    def block_of(s):
        j = s // 2
        hop = j + j // 2 - 2 * (j // 3)
        return lax.rem(me + 2 * hop, n) + lax.rem(s, 2) * other

    def gate_load(s, slot):
        r = rows(block_of(s))
        return (
            local(gate_ref.at[r], gu_v.at[slot, 0], g_sem.at[slot, 0]),
            local(up_ref.at[r], gu_v.at[slot, 1], g_sem.at[slot, 1]),
        )

    def tile_load(s, slot):
        return local(dyg.at[rows(block_of(s))], tile_v.at[slot], t_sem.at[slot])

    w_copies[0].start()
    local(dy_ref, tile_v.at[0], t_sem.at[0]).start()
    for c in gate_load(0, 0):
        c.start()
    stage = [local(dy_ref, psend.at[0], own_sem.at[0]), local(x_ref, psend.at[1], own_sem.at[1])]
    for c in stage:
        c.start()
    w_copies[1].start()
    w_copies[2].start()
    keep_own = [local(psend.at[0], dyg.at[rows(me)], own_sem.at[0]), local(psend.at[1], xg.at[rows(me)], own_sem.at[1])]
    w_copies[0].wait()

    def step(s, _):
        slot, nxt = lax.rem(s, 2), lax.rem(s + 1, 2)
        r = rows(block_of(s))
        tile_load(s, slot).wait()
        for c in gate_load(s, slot):
            c.wait()
        dh_v[...] = lax.dot_general(tile_v[slot], wd_v[...], NT, preferred_element_type=F32)

        @pl.when(s == 0)
        def _():
            for c in stage:
                c.wait()
            for c in keep_own:
                c.start()
            pair_arrived(0, -1)

        @pl.when(s == 1)
        def _():
            for k in (0, 2):
                ring_arrived(0, k)
            for k in (4, 5):
                ring_fwd(0, k).start()
            for k in (0, 2, 1, 3):
                ring_own(1, k).start()
            for k in (0, 2):
                pair_fwd(0, k).start()
            for k in (1, 3):
                ring_arrived(0, k)
                pair_fwd(0, k).start()

        @pl.when(s == 2)
        def _():
            for k in (2, 3):
                pair_arrived(0, k)

        @pl.when(s == 4)
        def _():
            for k in (0, 1):
                pair_arrived(0, k)

        @pl.when(s == 5)
        def _():
            for k in (4, 5):
                ring_arrived(0, k)
                pair_fwd(0, k).start()

        @pl.when(s == 6)
        def _():
            for k in (4, 5):
                pair_arrived(0, k)

        @pl.when(s < n - 1)
        def _():
            tile_load(s + 1, nxt).start()
            for c in gate_load(s + 1, nxt):
                c.start()

        def chunk(i, _):
            m = 16
            q = pl.ds(pl.multiple_of(i * m, m), m)
            o = pl.ds(pl.multiple_of(block_of(s) * R + i * m, m), m)
            hidden, back = jax.vjp(act, gu_v[slot, 0, q].astype(F32), gu_v[slot, 1, q].astype(F32))
            dg, du = back(dh_v[q])
            dgu_v[o, pl.ds(0, F)] = dg.astype(BF16)
            dgu_v[o, pl.ds(F, F)] = du.astype(BF16)
            hid_v[o] = hidden.astype(BF16)
            return 0

        lax.fori_loop(0, R // 16, chunk, 0)
        return 0

    lax.fori_loop(0, n, step, 0)
    for c in keep_own:
        c.wait()
    for c in w_copies[1:]:
        c.wait()

    W = strip_v.shape[2]

    def strip_load(a, t, slot):
        return local(full[a].at[:, pl.ds(pl.multiple_of(t * W, W), W)], strip_v.at[slot], st_sem.at[slot])

    NB = 512

    def dx_terms(row0, m, emit):
        def ntile(t, _):
            cols = pl.ds(pl.multiple_of(t * NB, NB), NB)
            emit(cols, lax.dot_general(dgu_v[pl.ds(row0, m)], wgu_v[cols], NT, preferred_element_type=F32))
            return 0

        lax.fori_loop(0, D // NB, ntile, 0)

    targets = (far, right, left, me)

    def p_copy(i):
        return remote(psend.at[i % 2], pbuf.at[i], p_s.at[i], p_r.at[i], partner)

    for i, block in enumerate(targets):
        if i >= 2:
            p_copy(i - 2).wait_send()

        def emit(cols, v, i=i):
            psend[i % 2, :, cols] = v.astype(BF16)

        dx_terms(pl.multiple_of((block + other) * R, R), R, emit)
        if i >= 1:
            p_copy(i - 1).start()

    for k in (0, 2):
        ring_arrived(1, k)
    for k in (4, 5):
        ring_fwd(1, k).start()
    for k in (0, 2):
        pair_fwd(1, k).start()
    p_copy(3).start()

    def p_load(i, half=None):
        if half is None:
            return local(pbuf.at[i], tile_v.at[i % 2], t_sem.at[i % 2])
        h = pl.ds(half * H, H)
        return local(pbuf.at[i, h], tile_v.at[i % 2, h], t_sem.at[i % 2])

    def p_fetch(i):
        p_copy(i).wait_recv()
        p_load(i).start()

    PIECE = H // C

    def q_src(q):
        return rsend.at[q] if q < 4 else last_v.at[q - 4]

    def q_part(q, sub=None):
        h, k = (pl.ds(0, H), q) if sub is None else (pl.ds(pl.multiple_of(sub * PIECE, PIECE), PIECE), q + 2 * sub)
        return remote(q_src(q).at[h], rrecv.at[q, h], q_s.at[k], q_r.at[k], (right, left)[q % 2])

    def q_parts(q):
        return [q_part(q)] if q < 4 else [q_part(q, sub) for sub in range(C)]

    def ring_sum(q, i, half, add=None):
        h = pl.ds(half * H, H)
        dst = q_src(q)

        def emit(cols, v):
            v = v + tile_v[i % 2, h, cols].astype(F32)
            if add is not None:
                v = v + rrecv[add, :, cols].astype(F32)
            dst[:, cols] = v.astype(BF16)

        dx_terms(pl.multiple_of(targets[i] * R + half * H, H), H, emit)
        if 1 <= q < 4:
            q_part(q - 1).start()

    p_fetch(0)
    p_fetch(1)
    p_load(0).wait()
    ring_sum(0, 0, 0)
    ring_sum(1, 0, 1)
    p_fetch(2)
    p_load(1).wait()
    ring_sum(2, 1, 1)
    p_fetch(3)
    p_load(2).wait()
    ring_sum(3, 2, 0)
    p_load(3).wait()

    def emit_own(cols, v):
        acc_v[:, cols] = v + tile_v[1, :, cols].astype(F32)

    strip_load(0, 0, 0).start()
    dx_terms(pl.multiple_of(me * R, R), R, emit_own)
    q_part(3).start()

    for k in (1, 3):
        ring_arrived(1, k)
        pair_fwd(1, k).start()

    def strips(a, lo, hi, work, after_first=lambda: None):
        def one(t, _):
            slot = lax.rem(t, 2)
            strip_load(a, t, slot).wait()

            @pl.when(t + 1 < hi)
            def _():
                strip_load(a, t + 1, 1 - slot).start()

            work(slot, pl.ds(pl.multiple_of(t * W, W), W))
            pl.when(t == lo)(after_first)
            return 0

        lax.fori_loop(lo, hi, one, 0)

    def down_work(slot, part):
        v = lax.dot_general(strip_v[slot], hid_v[...], TN, preferred_element_type=F32)
        dwd_ref[:, part] = v.T.astype(BF16)

    def in_work(slot, part):
        v = lax.dot_general(strip_v[slot], dgu_v[...], TN, preferred_element_type=F32)
        dwg_ref[part] = v[:, :F].astype(BF16)
        dwu_ref[part] = v[:, F:].astype(BF16)

    S = D // W
    strips(0, 0, S, down_work)

    for k in (4, 5):
        ring_arrived(1, k)
        pair_fwd(1, k).start()
    for k in (-1, 0, 1, 2, 3, 4, 5):
        pair_arrived(1, k)

    strip_load(1, 0, 0).start()
    for i, half in ((1, 0), (2, 1)):
        p_load(i, half).start()
    strips(1, 0, S // 2, in_work)

    strip_load(1, S // 2, S // 2 % 2).start()
    for c in q_parts(0) + q_parts(1):
        c.wait_recv()
    for i, half in ((1, 0), (2, 1)):
        p_load(i, half).wait()
    for i in (2, 3):
        p_copy(i).wait_send()
    ring_sum(4, 1, 0, add=0)
    ring_sum(5, 2, 1, add=1)

    def send_last():
        @pl.when(core == 1)
        def _():
            for sub in range(C):
                for q in (4, 5):
                    q_part(q, sub).start()

    strips(1, S // 2, S, in_work, send_last)

    for a in range(2):
        for k in range(4):
            ring_own(a, k).wait_send()
        pair_own(a).wait_send()
        for k in (4, 5):
            ring_fwd(a, k).wait_send()
        for k in range(6):
            pair_fwd(a, k).wait_send()
    for q in range(4):
        q_part(q).wait_send()
    for q in (2, 3):
        q_part(q).wait_recv()

    def settle(i, _):
        h = pl.ds(pl.multiple_of(i * 16, 16), 16)
        for q, base in ((3, 0), (2, H)):
            r = pl.ds(pl.multiple_of(base + i * 16, 16), 16)
            acc_v[r] = acc_v[r] + rrecv[q, h].astype(F32)
        return 0

    lax.fori_loop(0, H // 16, settle, 0)

    @pl.when(core == 1)
    def _():
        def finish(sub, _):
            for q, base in ((4, 0), (5, H)):
                q_part(q, sub).wait_recv()

                def put(i, _):
                    h = pl.ds(pl.multiple_of(sub * PIECE + i * 16, 16), 16)
                    r = pl.ds(pl.multiple_of(base + sub * PIECE + i * 16, 16), 16)
                    acc_v[r] = acc_v[r] + rrecv[q, h].astype(F32)
                    return 0

                lax.fori_loop(0, PIECE // 16, put, 0)
            for q in (4, 5):
                q_part(q, sub).wait_send()
            return 0

        lax.fori_loop(0, C, finish, 0)


def last_hop(n, acc_v, last_v, after_ref, dx_ref, recv_v, s_sem, r_sem):
    me = lax.axis_index("tp")
    core = lax.rem(me, 2)
    to = (lax.rem(me + 2, n), lax.rem(me + n - 2, n))
    H = acc_v.shape[0] // 2
    PIECE = H // C

    barrier = pltpu.get_barrier_semaphore()
    for t in to:
        pl.semaphore_signal(barrier, inc=1, device_id={"tp": t}, device_id_type=MESH)
    pl.semaphore_wait(barrier, 2)

    def part(q, sub):
        h = pl.ds(pl.multiple_of(sub * PIECE, PIECE), PIECE)
        return pltpu.make_async_remote_copy(
            src_ref=last_v.at[q, h], dst_ref=recv_v.at[q, h], send_sem=s_sem.at[q, sub], recv_sem=r_sem.at[q, sub],
            device_id={"tp": to[q]}, device_id_type=MESH,
        )

    def finish(lo, count, add, halves=(0, 1)):
        for q in halves:
            def put(i, _):
                h = pl.ds(pl.multiple_of(lo + i * 16, 16), 16)
                r = pl.ds(pl.multiple_of(q * H + lo + i * 16, 16), 16)
                v = acc_v[r]
                if add:
                    v = v + recv_v[q, h].astype(F32)
                dx_ref[r] = v.astype(BF16)
                return 0

            lax.fori_loop(0, count // 16, put, 0)

    @pl.when(core == 0)
    def _():
        for sub in range(C):
            for q in range(2):
                part(q, sub).start()

        def each(sub, _):
            for q in range(2):
                part(q, sub).wait_send()
            for q in range(2):
                part(q, sub).wait_recv()
                finish(sub * PIECE, PIECE, True, (q,))
            return 0

        lax.fori_loop(0, C, each, 0)

    @pl.when(core == 1)
    def _():
        finish(0, H, False)


def write_out(*refs):
    k = (len(refs) - 2) // 2
    refs[-2][...] = jnp.zeros_like(refs[-2])
    copies = [pltpu.make_async_copy(refs[i], refs[k + i], refs[-1].at[i]) for i in range(k)]
    for c in copies:
        c.start()
    for c in copies:
        c.wait()


def solution(mesh):
    n = mesh.shape["tp"]

    def body(x, dy, gate, up, w_gate, w_up, w_down):
        R, D = x.shape
        T, F = gate.shape
        H = R // 2
        W = 256
        out = lambda *s: jax.ShapeDtypeStruct(s, BF16)
        vmem_spec = pl.BlockSpec(memory_space=pltpu.VMEM)
        any_spec = pl.BlockSpec(memory_space=pl.ANY)
        dma = pltpu.SemaphoreType.DMA
        vmem = lambda s, t: pltpu.VMEM(s, t)
        keep = lambda a: pltpu.with_memory_space_constraint(a, pltpu.VMEM)

        *dw, acc, last, _, _, _ = pl.pallas_call(
            functools.partial(kernel, n),
            out_shape=[vmem(s, BF16) for s in ((D, F), (D, F), (F, D))]
            + [vmem((R, D), F32), vmem((2, H, D), BF16), out(T, D), out(T, D), out(4, R, D)],
            in_specs=[any_spec] * 7,
            out_specs=[vmem_spec] * 5 + [any_spec] * 3,
            scratch_shapes=[
                pltpu.VMEM((D, 2 * F), BF16),
                pltpu.VMEM((T, 2 * F), BF16),
                pltpu.VMEM((T, F), BF16),
                pltpu.VMEM((2, R, D), BF16),
                pltpu.VMEM((2, 2, R, F), BF16),
                pltpu.VMEM((R, F), F32),
                pltpu.VMEM((2, R, D), BF16),
                pltpu.VMEM((4, H, D), BF16),
                pltpu.VMEM((6, H, D), BF16),
                pltpu.VMEM((2, T, W), BF16),
                pltpu.SemaphoreType.REGULAR,
                dma((2, 13)), dma((2, 13)),
                dma((4,)), dma((4,)),
                dma((4 + 2 * C,)), dma((4 + 2 * C,)),
                dma((3,)), dma((2, 2)), dma((2,)), dma((2,)),
                dma((2,)),
            ],
            compiler_params=pltpu.CompilerParams(collective_id=0, has_side_effects=True, vmem_limit_bytes=199 * 2**18),
            name="mlp_backward",
        )(x, dy, gate, up, w_gate, w_up, w_down)
        *dw, written = pl.pallas_call(
            write_out,
            out_shape=[out(*a.shape) for a in dw] + [vmem((8, 128), F32)],
            in_specs=[vmem_spec] * len(dw),
            out_specs=[any_spec] * len(dw) + [vmem_spec],
            scratch_shapes=[dma((len(dw),))],
            compiler_params=pltpu.CompilerParams(vmem_limit_bytes=2**18),
            name="write_weight_gradients",
        )(*(keep(a) for a in dw))
        dx = pl.pallas_call(
            functools.partial(last_hop, n),
            out_shape=vmem((R, D), BF16),
            in_specs=[vmem_spec] * 3,
            out_specs=vmem_spec,
            scratch_shapes=[pltpu.VMEM((2, H, D), BF16), dma((2, C)), dma((2, C))],
            compiler_params=pltpu.CompilerParams(collective_id=1, has_side_effects=True, vmem_limit_bytes=2**22),
            name="last_hop",
        )(keep(acc), keep(last), keep(written))
        return (dx, *dw)

    tok, col, row = P(("dp", "tp"), None), P("dp", "tp"), P("tp", None)
    wcol = P(None, "tp")
    return jax.shard_map(
        body, mesh=mesh, in_specs=(tok, tok, col, col, wcol, wcol, row), out_specs=(tok, col, col, tok), check_vma=False
    )
```
